32 devices in a mesh: dp: 1 (over z), tp: 32 (over y, x, core).
Axes of the slice: x: 4, y: 4, z: 1, core: 2. Of those that a mesh axis runs over, the one named last changes fastest.
The devices are a block of a 4x4x8 slice.
Arguments:
- hidden: bfloat16 [4096, 512], P(('dp', 'tp'))
- targets: int32 [4096], P(('dp', 'tp'))
- loss_mask: int32 [4096], P(('dp', 'tp'))
- ln_params: float32 [2, 512], replicated
- out_embed: bfloat16 [50304, 512], P('tp')
- ln_mom1: float32 [2, 512], replicated
- ln_mom2: float32 [2, 512], replicated
- embed_mom1: float32 [50304, 512], P('tp')
- embed_mom2: float32 [50304, 512], P('tp')
Outputs:
- output 1: float32 [4096], P(('dp', 'tp'))
- output 2: float32 [1], P('dp')
- output 3: bfloat16 [4096, 512], P(('dp', 'tp'))
- output 4: float32 [2, 512], P('dp')
- output 5: float32 [2, 512], P('dp')
- output 6: float32 [2, 512], P('dp')
- output 7: bfloat16 [50304, 512], P(('dp', 'tp'))
- output 8: float32 [50304, 512], P(('dp', 'tp'))
- output 9: float32 [50304, 512], P(('dp', 'tp'))
All inputs are finite; a program needn't handle non-finite values.
Results may differ from the reference program's by a relative error of at most 0.001.
Values are sent between devices in bfloat16 or wider.
A program may use at most 768 MiB of HBM per device.

```python
import math
import jax
import jax.numpy as jnp
from jax import lax

MODEL_DIM = 512
VOCAB_SIZE = 50304
SEQ_LEN = 4096
ADAM_STEP = 10
ROW_BLOCK = math.gcd(SEQ_LEN, 256)
NUM_BLOCKS = SEQ_LEN // ROW_BLOCK
LN_EPS = 1e-5
BETA_ONE = 0.9
BETA_TWO = 0.95
ADAM_EPS = 1e-8
LEARN_RATE = 1e-3
WEIGHT_DECAY = 0.1


def setup_inputs(seed: int = 0, part: int = 0) -> dict:
    root_key = jax.random.key(seed)
    shared_keys = jax.random.split(root_key, 6)
    part_keys = jax.random.split(jax.random.fold_in(root_key, part), 4)
    hidden = jax.random.normal(part_keys[0], (SEQ_LEN, MODEL_DIM), jnp.float32).astype(jnp.bfloat16)
    targets = jax.random.randint(part_keys[1], (SEQ_LEN,), 0, VOCAB_SIZE, jnp.int32)
    keep_bits = jax.random.randint(part_keys[2], (SEQ_LEN,), 0, 4, jnp.int32)
    pad_len = jax.random.randint(part_keys[3], (), 0, SEQ_LEN // 4, jnp.int32)
    positions = jnp.arange(SEQ_LEN, dtype=jnp.int32)
    keep_tok = (keep_bits > 0) & (positions < SEQ_LEN - pad_len)
    loss_mask = jnp.where(positions == 0, 1, keep_tok.astype(jnp.int32)).astype(jnp.int32)
    embed_scale = 2.3 * MODEL_DIM ** -0.5
    out_embed = (jax.random.normal(shared_keys[0], (VOCAB_SIZE, MODEL_DIM), jnp.float32) * embed_scale).astype(jnp.bfloat16)
    ln_noise = jax.random.normal(shared_keys[1], (2, MODEL_DIM), jnp.float32)
    ln_params = jnp.stack([1.0 + 0.3 * ln_noise[0], 0.3 * ln_noise[1]])
    valid_est = 0.66 * SEQ_LEN
    embed_grad = (valid_est * VOCAB_SIZE) ** -0.5
    ln_grad = 2.3 * (valid_est * MODEL_DIM) ** -0.5
    ln_mom1 = jax.random.normal(shared_keys[2], (2, MODEL_DIM), jnp.float32) * ln_grad
    ln_mom2 = (0.5 + jax.random.uniform(shared_keys[3], (2, MODEL_DIM), jnp.float32)) * ln_grad ** 2
    embed_mom1 = jax.random.normal(shared_keys[4], (VOCAB_SIZE, MODEL_DIM), jnp.float32) * embed_grad
    embed_mom2 = (0.5 + jax.random.uniform(shared_keys[5], (VOCAB_SIZE, MODEL_DIM), jnp.float32)) * embed_grad ** 2
    return {"hidden": hidden, "targets": targets, "loss_mask": loss_mask, "ln_params": ln_params, "out_embed": out_embed, "ln_mom1": ln_mom1, "ln_mom2": ln_mom2, "embed_mom1": embed_mom1, "embed_mom2": embed_mom2}


def layer_norm(hidden, ln_params):
    rows_f32 = hidden.astype(jnp.float32)
    row_mean = jnp.mean(rows_f32, axis=-1, keepdims=True)
    centered = rows_f32 - row_mean
    row_var = jnp.mean(centered * centered, axis=-1, keepdims=True)
    normed = centered * lax.rsqrt(row_var + LN_EPS)
    return normed * ln_params[0] + ln_params[1]


def adam_step(param_val, grad_val, m_old, v_old, decay_rate):
    m_new = BETA_ONE * m_old + (1.0 - BETA_ONE) * grad_val
    v_new = BETA_TWO * v_old + (1.0 - BETA_TWO) * grad_val * grad_val
    m_hat = m_new / (1.0 - BETA_ONE ** ADAM_STEP)
    v_hat = v_new / (1.0 - BETA_TWO ** ADAM_STEP)
    new_param = param_val - LEARN_RATE * (m_hat / (jnp.sqrt(v_hat) + ADAM_EPS) + decay_rate * param_val)
    return new_param, m_new, v_new


def block_logits(x_block, out_embed):
    return jnp.dot(x_block, out_embed.T, preferred_element_type=jnp.float32)


def reference(hidden, targets, loss_mask, ln_params, out_embed, ln_mom1, ln_mom2, embed_mom1, embed_mom2):
    x_norm, ln_vjp = jax.vjp(layer_norm, hidden, ln_params)
    x_bf = x_norm.astype(jnp.bfloat16)
    mask_f = loss_mask.astype(jnp.float32)
    valid_count = jnp.sum(mask_f)
    vocab_ids = jnp.arange(VOCAB_SIZE, dtype=jnp.int32)
    x_blocks = x_bf.reshape(NUM_BLOCKS, ROW_BLOCK, MODEL_DIM)
    tgt_blocks = targets.reshape(NUM_BLOCKS, ROW_BLOCK)
    scale_blocks = (mask_f / valid_count).reshape(NUM_BLOCKS, ROW_BLOCK)

    def forward_block(block_in):
        x_block, tgt_block = block_in
        logits = block_logits(x_block, out_embed)
        lse_block = jax.nn.logsumexp(logits, axis=-1)
        is_target = vocab_ids[None, :] == tgt_block[:, None]
        tgt_logit = jnp.sum(jnp.where(is_target, logits, 0.0), axis=-1)
        return lse_block, tgt_logit

    lse_blocks, tgt_logits = lax.map(forward_block, (x_blocks, tgt_blocks))
    token_loss = (lse_blocks.reshape(SEQ_LEN) - tgt_logits.reshape(SEQ_LEN)) * mask_f
    mean_loss = (jnp.sum(token_loss) / valid_count).reshape(1)

    def backward_block(d_embed, block_in):
        x_block, tgt_block, lse_block, scale_block = block_in
        logits = block_logits(x_block, out_embed)
        prob_vals = jnp.exp(logits - lse_block[:, None])
        is_target = (vocab_ids[None, :] == tgt_block[:, None]).astype(jnp.float32)
        d_logits = ((prob_vals - is_target) * scale_block[:, None]).astype(jnp.bfloat16)
        d_embed = d_embed + jnp.dot(d_logits.T, x_block, preferred_element_type=jnp.float32)
        d_x = jnp.dot(d_logits, out_embed, preferred_element_type=jnp.float32)
        return d_embed, d_x

    d_embed, d_x = lax.scan(backward_block, jnp.zeros((VOCAB_SIZE, MODEL_DIM), jnp.float32), (x_blocks, tgt_blocks, lse_blocks, scale_blocks))
    d_hidden, d_ln = ln_vjp(d_x.reshape(SEQ_LEN, MODEL_DIM))
    ln_new, ln_mom1_new, ln_mom2_new = adam_step(ln_params, d_ln, ln_mom1, ln_mom2, 0.0)
    embed_f, embed_mom1_new, embed_mom2_new = adam_step(out_embed.astype(jnp.float32), d_embed, embed_mom1, embed_mom2, WEIGHT_DECAY)
    return (token_loss, mean_loss, d_hidden, ln_new, ln_mom1_new, ln_mom2_new, embed_f.astype(jnp.bfloat16), embed_mom1_new, embed_mom2_new)
```

```python
import functools
import math

import jax
import jax.numpy as jnp
from jax import lax
from jax.experimental import pallas as pl
from jax.experimental.pallas import tpu as pltpu
from jax.sharding import PartitionSpec as P

LN_EPS = 1e-5
BETA_ONE = 0.9
BETA_TWO = 0.95
ADAM_EPS = 1e-8
LEARN_RATE = 1e-3
WEIGHT_DECAY = 0.1
ADAM_STEP = 10
MESH = pl.DeviceIdType.MESH
CORES = 2
PAIR = (0, 1)
LAST = (2, 3)
ANY = pl.BlockSpec(memory_space=pl.ANY)
VMEM = pl.BlockSpec(memory_space=pltpu.VMEM)
F32, BF16 = jnp.float32, jnp.bfloat16
NN = (((1,), (0,)), ((), ()))
NT = (((1,), (1,)), ((), ()))


def adam_step(param_val, grad_val, m_old, v_old, decay_rate):
    m_new = BETA_ONE * m_old + (1.0 - BETA_ONE) * grad_val
    v_new = BETA_TWO * v_old + (1.0 - BETA_TWO) * grad_val * grad_val
    m_hat = m_new / (1.0 - BETA_ONE ** ADAM_STEP)
    v_hat = v_new / (1.0 - BETA_TWO ** ADAM_STEP)
    new_param = param_val - LEARN_RATE * (m_hat / (jnp.sqrt(v_hat) + ADAM_EPS) + decay_rate * param_val)
    return new_param, m_new, v_new


def row_tiles(rows, size):
    return [(r, min(size, rows - r)) for r in range(0, rows, size)]


def step_kernel(side, hid_ref, tgt_ref, msk_ref, lnp_ref, emb_ref,
                dE_out, dh_out, dln_out, loss_out, mean_out,
                xg, ee, et, ez, dz, dxp, r1, r2, t2, q1, q2,
                tm_all, st_all, tgt_ck, msk_ck, rel_ck, a_ck, s_ck, loss_ck, pair, dl_all, fin,
                loc_sem, ag_s, ag_r, tm_s, tm_r, st_s, st_r, rs_s, rs_r, dl_s, dl_r, pr_s, pr_r, free_sem):
    chips = side * side
    ndev = chips * CORES
    tok = hid_ref.shape[0]
    half = tok // 2
    dim = hid_ref.shape[1]
    voc = emb_ref.shape[0]
    ct = half * side
    nck = 2 * side
    hd = dim // 2
    me = lax.axis_index("tp")
    core = lax.rem(me, CORES)
    chip = me // CORES
    mx, my = lax.rem(chip, side), chip // side
    sib = me + 1 - 2 * core

    def dev(y, x):
        return {"tp": (lax.rem(y, side) * side + lax.rem(x, side)) * CORES + core}

    def dev_minor(g, d):
        return dev(my, mx + d) if g == 0 else dev(my + d, mx)

    def dev_major(g, d):
        return dev(my + d, mx) if g == 0 else dev(my, mx + d)

    maj = (my, mx)
    mnr = (mx, my)

    def chunk_of(g, d):
        return g * side + lax.rem(maj[g] + d, side)

    def rcopy(src, dst, ssem, rsem, device):
        return pltpu.make_async_remote_copy(src_ref=src, dst_ref=dst, send_sem=ssem, recv_sem=rsem,
                                            device_id=device, device_id_type=MESH)

    e_local = pltpu.make_async_copy(emb_ref, ee.at[0], loc_sem.at[0])
    e_local.start()
    barrier = pltpu.get_barrier_semaphore()
    for d in range(1, ndev):
        pl.semaphore_signal(barrier, inc=1, device_id={"tp": lax.rem(me + d, ndev)}, device_id_type=MESH)

    rows = hid_ref[...].astype(F32)
    cent = rows - jnp.mean(rows, axis=-1, keepdims=True)
    rstd = lax.rsqrt(jnp.mean(cent * cent, axis=-1, keepdims=True) + LN_EPS)
    xb = (cent * rstd * lnp_ref[0:1, :] + lnp_ref[1:2, :]).astype(BF16)

    def xslot(c, pos, r0=0, n=half):
        return xg.at[pl.ds(pl.multiple_of(c * ct + pos * half + r0, 32), n)]

    for g in PAIR:
        xslot_rows = pl.ds(pl.multiple_of(chunk_of(g, 0) * ct + mnr[g] * half, half), half)
        xg[xslot_rows, :] = xb[g * half:(g + 1) * half]
    tm_all[chip, 0:1, :] = tgt_ref[...]
    tm_all[chip, 1:2, :] = msk_ref[...]
    tm_all[chip, 2:8, :] = jnp.zeros((6, tok), jnp.int32)
    et[:, :, voc:] = jnp.zeros((2, dim, et.shape[2] - voc), BF16)

    pl.semaphore_wait(barrier, ndev - 1)

    def ag1(g, k):
        c, p = chunk_of(g, 0), mnr[g]
        if k < 2:
            s = xslot(c, p)
            return rcopy(s, s, ag_s.at[g, 0, k], ag_r.at[g, 0, k], dev_minor(g, (1, side - 1)[k]))
        q = lax.rem(p + (side - 1, 1)[k - 2], side)
        s = xslot(c, q, (0, half // 2)[k - 2], half // 2)
        return rcopy(s, s, ag_s.at[g, 0, k], ag_r.at[g, 0, k], dev_minor(g, (1, side - 1)[k - 2]))

    def ag1_recv(g, k):
        c, p = chunk_of(g, 0), mnr[g]
        if k < 2:
            s = xslot(c, lax.rem(p + (side - 1, 1)[k], side))
        else:
            s = xslot(c, lax.rem(p + 2, side), (0, half // 2)[k - 2], half // 2)
        rcopy(s, s, ag_s.at[g, 0, k], ag_r.at[g, 0, k], dev_minor(g, 1)).wait_recv()

    def cslot(c, r0, n):
        return xg.at[pl.ds(pl.multiple_of(c * ct + r0, 32), n)]

    def ag2(g, k):
        if k < 2:
            s = cslot(chunk_of(g, 0), 0, ct)
            return rcopy(s, s, ag_s.at[g, 1, k], ag_r.at[g, 1, k], dev_major(g, (1, side - 1)[k]))
        s = cslot(chunk_of(g, (side - 1, 1)[k - 2]), (0, ct // 2)[k - 2], ct // 2)
        return rcopy(s, s, ag_s.at[g, 1, k], ag_r.at[g, 1, k], dev_major(g, (1, side - 1)[k - 2]))

    def ag2_recv(g, k):
        if k < 2:
            s = cslot(chunk_of(g, (side - 1, 1)[k]), 0, ct)
        else:
            s = cslot(chunk_of(g, 2), (0, ct // 2)[k - 2], ct // 2)
        rcopy(s, s, ag_s.at[g, 1, k], ag_r.at[g, 1, k], dev_major(g, 1)).wait_recv()

    for k in PAIR:
        for g in PAIR:
            ag1(g, k).start()
    e_send = rcopy(emb_ref, ee.at[1], pr_s.at[0], pr_r.at[0], {"tp": sib})
    e_send.start()
    tms = []
    for d in range(1, chips):
        t = lax.rem(chip + d, chips)
        cp = rcopy(tm_all.at[chip], tm_all.at[chip], tm_s.at[d], tm_r.at[d], {"tp": t * CORES + core})
        cp.start()
        tms.append(cp)

    for k in PAIR:
        for g in PAIR:
            ag1_recv(g, k)
            ag1(g, k + 2).start()

    def transpose_e(h):
        for r0, n in row_tiles(voc, 384):
            et[h, :, r0:r0 + n] = ee[h, r0:r0 + n, :].T

    e_local.wait()
    transpose_e(0)

    for k in LAST:
        for g in PAIR:
            ag1_recv(g, k)
    for k in PAIR:
        for g in PAIR:
            ag2(g, k).start()

    for d in range(1, chips):
        s = tm_all.at[lax.rem(chip + chips - d, chips)]
        rcopy(s, s, tm_s.at[d], tm_r.at[d], {"tp": me}).wait_recv()
    lane = lax.broadcasted_iota(jnp.int32, (8, tok), 1)
    for c in range(nck):
        for j in range(ct // tok):
            if c < side:
                a, b = tm_all[c * side + 2 * j], tm_all[c * side + 2 * j + 1]
                v = jnp.where(lane < half, a, pltpu.roll(b, half, 1))
            else:
                a, b = tm_all[2 * j * side + c - side], tm_all[(2 * j + 1) * side + c - side]
                v = jnp.where(lane < half, pltpu.roll(a, half, 1), b)
            tgt_ck[c:c + 1, j * tok:(j + 1) * tok] = v[0:1]
            msk_ck[c:c + 1, j * tok:(j + 1) * tok] = v[1:2]
    own = tgt_ck[...] - me * voc
    oth = tgt_ck[...] - sib * voc
    rel_ck[0] = own
    rel_ck[1] = oth
    maskf = msk_ck[...].astype(F32)
    cnt = jnp.sum(maskf, keepdims=True)
    pair[0] = jnp.broadcast_to(cnt, (8, tok))
    cnt_send = rcopy(pair.at[0], pair.at[1], pr_s.at[1], pr_r.at[1], {"tp": sib})
    cnt_send.start()

    e_send.wait_recv()
    transpose_e(1)

    def logits_chunk(c):
        x_c = xg[pl.ds(pl.multiple_of(c * ct, ct), ct), :]
        pair_i, lane0 = c // 2, pl.multiple_of(lax.rem(c, 2) * ct, ct)
        top = None
        for h in PAIR:
            for r0, n in row_tiles(voc, 528):
                z = lax.dot_general(ee[h, r0:r0 + n, :], x_c, NT, preferred_element_type=F32)
                ez[pair_i, h, r0:r0 + n, pl.ds(lane0, ct)] = z
                t = jnp.max(z, axis=0, keepdims=True)
                top = t if top is None else jnp.maximum(top, t)
        tot = jnp.zeros((1, ct), F32)
        tl = jnp.zeros((1, ct), F32)
        for h in PAIR:
            rel = rel_ck[h, pl.ds(c, 1), :]
            for r0, n in row_tiles(voc, 528):
                z = ez[pair_i, h, r0:r0 + n, pl.ds(lane0, ct)]
                e = jnp.exp(z - top)
                ez[pair_i, h, r0:r0 + n, pl.ds(lane0, ct)] = e
                tot += jnp.sum(e, axis=0, keepdims=True)
                hit = lax.broadcasted_iota(jnp.int32, (n, ct), 0) == rel - r0
                tl += jnp.sum(jnp.where(hit, z, 0.0), axis=0, keepdims=True)
        st_all[chip, 0, pl.ds(c, 1), :] = top
        st_all[chip, 1, pl.ds(c, 1), :] = tot
        st_all[chip, 2, pl.ds(c, 1), :] = tl

    def both(fn, d):
        def body(g, carry):
            m = my + g * (mx - my)
            fn(g * side + lax.rem(m + d, side))
            return carry
        lax.fori_loop(0, 2, body, 0)

    both(logits_chunk, 0)
    for k in PAIR:
        for g in PAIR:
            ag2_recv(g, k)
            ag2(g, k + 2).start()
    both(logits_chunk, 1)
    both(logits_chunk, side - 1)
    for k in LAST:
        for g in PAIR:
            ag2_recv(g, k)
    both(logits_chunk, 2)

    sts = []
    for d in range(1, chips):
        t = lax.rem(chip + d, chips)
        cp = rcopy(st_all.at[chip], st_all.at[chip], st_s.at[d], st_r.at[d], {"tp": t * CORES + core})
        cp.start()
        sts.append(cp)
    rcopy(pair.at[0], pair.at[1], pr_s.at[1], pr_r.at[1], {"tp": sib}).wait_recv()
    total_n = (pair[0] + pair[1])[0:1, 0:1]
    scale = maskf / total_n
    s_ck[...] = scale
    for d in range(1, chips):
        s = st_all.at[lax.rem(chip + chips - d, chips)]
        rcopy(s, s, st_s.at[d], st_r.at[d], {"tp": me}).wait_recv()
    gmax = st_all[0, 0]
    for t in range(1, chips):
        gmax = jnp.maximum(gmax, st_all[t, 0])
    gsum = jnp.zeros_like(gmax)
    gtl = jnp.zeros_like(gmax)
    for t in range(chips):
        gsum += st_all[t, 1] * jnp.exp(st_all[t, 0] - gmax)
        gtl += st_all[t, 2]
    lse = gmax + jnp.log(gsum)
    a_ck[...] = jnp.exp(st_all[chip, 0] - lse) * scale
    loss = (lse - gtl) * maskf
    loss_ck[...] = loss
    lsum = jnp.sum(loss, keepdims=True)
    pair[2] = jnp.broadcast_to(lsum, (8, tok))
    loss_send = rcopy(pair.at[2], pair.at[3], pr_s.at[2], pr_r.at[2], {"tp": sib})
    loss_send.start()

    def grad_chunk(c):
        pair_i, lane0 = c // 2, pl.multiple_of(lax.rem(c, 2) * ct, ct)
        out0 = pl.multiple_of(c * ct, ct)
        a = a_ck[pl.ds(c, 1), :]
        s = s_ck[pl.ds(c, 1), :]
        acc = None
        for h in PAIR:
            rel = rel_ck[h, pl.ds(c, 1), :]
            for r0, n in row_tiles(voc, 528):
                e = ez[pair_i, h, r0:r0 + n, pl.ds(lane0, ct)]
                hit = lax.broadcasted_iota(jnp.int32, (n, ct), 0) == rel - r0
                dz[h, r0:r0 + n, pl.ds(out0, ct)] = (e * a - jnp.where(hit, s, 0.0)).astype(BF16)
        for q in range(2):
            acc = None
            for h in PAIR:
                t = lax.dot_general(et[h, q * hd:(q + 1) * hd, :], dz[h, :, pl.ds(out0, ct)], NN,
                                    preferred_element_type=F32)
                acc = t if acc is None else acc + t
            dxp[c, q * hd:(q + 1) * hd, :] = acc

    dz[:, voc:, :] = jnp.zeros((2, dz.shape[1] - voc, dz.shape[2]), BF16)

    class Ring:
        def __init__(self, stage, g, piece, relay, land, device):
            self.piece, self.relay, self.land, self.device = piece, relay, land, device
            self.ss, self.rr = rs_s.at[stage, g], rs_r.at[stage, g]
        def copy(self, k):
            minus, plus = side - 1, 1
            src, dst, to = {
                0: (lambda: self.piece(2, 0), lambda: self.relay(0), minus),
                1: (lambda: self.piece(2, 1), lambda: self.relay(1), plus),
                2: (lambda: self.piece(1, 0), lambda: self.land(1), plus),
                3: (lambda: self.piece(minus, 1), lambda: self.land(2), minus),
                4: (lambda: self.piece(minus, 0), lambda: self.land(0), minus),
                5: (lambda: self.piece(1, 1), lambda: self.land(3), plus),
            }[k]
            return rcopy(src(), dst(), self.ss.at[k], self.rr.at[k], self.device(to))

    def piece1(g):
        return lambda d, q: dxp.at[chunk_of(g, d), pl.ds(q * hd, hd)]

    def piece2(g):
        return lambda d, q: t2.at[g, pl.ds(pl.multiple_of(lax.rem(mnr[g] + d, side) * half + q * (half // 2), 32), half // 2)]

    ring1 = [Ring(0, g, piece1(g), lambda i, g=g: r1.at[g, i], lambda i, g=g: r2.at[g, i],
                  functools.partial(dev_major, g)) for g in PAIR]
    ring2 = [Ring(1, g, piece2(g), lambda i, g=g: q1.at[g, i], lambda i, g=g: q2.at[g, i],
                  functools.partial(dev_minor, g)) for g in PAIR]

    both(grad_chunk, 2)
    for k in PAIR:
        for g in PAIR:
            ring1[g].copy(k).start()
    both(grad_chunk, 1)
    for g in PAIR:
        ring1[g].copy(2).start()
    both(grad_chunk, side - 1)
    for g in PAIR:
        ring1[g].copy(3).start()
    for g in PAIR:
        ring1[g].copy(0).wait_recv()
        c = chunk_of(g, side - 1)
        dxp[c, 0:hd, :] = dxp[c, 0:hd, :] + r1[g, 0]
        ring1[g].copy(4).start()
        ring1[g].copy(1).wait_recv()
        c = chunk_of(g, 1)
        dxp[c, hd:, :] = dxp[c, hd:, :] + r1[g, 1]
        ring1[g].copy(5).start()
    both(grad_chunk, 0)
    pl.semaphore_signal(free_sem, inc=1, device_id={"tp": sib}, device_id_type=MESH)

    def embed_grad(h, dst):
        for r0, n in row_tiles(voc, 528):
            ez[0, dst, r0:r0 + n, :] = lax.dot_general(dz[h, r0:r0 + n, :], xg[...], NN, preferred_element_type=F32)

    embed_grad(1, 0)
    pl.semaphore_wait(free_sem, 1)
    de_send = rcopy(ez.at[0, 0], ez.at[1, 0], pr_s.at[3], pr_r.at[3], {"tp": sib})
    de_send.start()

    for g in PAIR:
        for k in range(2, 6):
            ring1[g].copy(k).wait_recv()
        c = chunk_of(g, 0)
        lo = dxp[c, 0:hd, :] + r2[g, 0] + r2[g, 1]
        hi = dxp[c, hd:, :] + r2[g, 2] + r2[g, 3]
        t2[g, :, 0:hd] = lo.T
        t2[g, :, hd:] = hi.T
        for k in range(4):
            ring2[g].copy(k).start()

    embed_grad(0, 1)
    de_send.wait_recv()
    for r0, n in row_tiles(voc, 528):
        ez[0, 1, r0:r0 + n, :] = ez[0, 1, r0:r0 + n, :] + ez[1, 0, r0:r0 + n, :]
    de_out = pltpu.make_async_copy(ez.at[0, 1], dE_out, loc_sem.at[1])
    de_out.start()

    hq = half // 2
    for g in PAIR:
        for k, d, q, to in ((0, side - 1, 0, 4), (1, 1, 1, 5)):
            ring2[g].copy(k).wait_recv()
            rs = pl.ds(pl.multiple_of(lax.rem(mnr[g] + d, side) * half + q * hq, 32), hq)
            t2[g, rs, :] = t2[g, rs, :] + q1[g, k]
            ring2[g].copy(to).start()
    for g in PAIR:
        for k in range(2, 6):
            ring2[g].copy(k).wait_recv()
        base = pl.multiple_of(mnr[g] * half, half)
        fin[g * half:g * half + hq, :] = t2[g, pl.ds(base, hq), :] + q2[g, 0] + q2[g, 1]
        fin[g * half + hq:(g + 1) * half, :] = t2[g, pl.ds(base + hq, hq), :] + q2[g, 2] + q2[g, 3]

    dx = fin[...]
    rows = hid_ref[...].astype(F32)
    cent = rows - jnp.mean(rows, axis=-1, keepdims=True)
    rstd = lax.rsqrt(jnp.mean(cent * cent, axis=-1, keepdims=True) + LN_EPS)
    normed = cent * rstd
    dgam = jnp.sum(dx * normed, axis=0, keepdims=True)
    dbet = jnp.sum(dx, axis=0, keepdims=True)
    for j in range(dim // tok):
        dl_all[me, j:j + 1, :] = dgam[:, j * tok:(j + 1) * tok]
        dl_all[me, 4 + j:5 + j, :] = dbet[:, j * tok:(j + 1) * tok]
    dls = []
    for d in range(1, ndev):
        cp = rcopy(dl_all.at[me], dl_all.at[me], dl_s.at[d], dl_r.at[d], {"tp": lax.rem(me + d, ndev)})
        cp.start()
        dls.append(cp)
    dn = dx * lnp_ref[0:1, :]
    dh = rstd * (dn - jnp.mean(dn, axis=-1, keepdims=True) - normed * jnp.mean(dn * normed, axis=-1, keepdims=True))
    dh_out[...] = dh.astype(BF16)

    lane1 = lax.broadcasted_iota(jnp.int32, (1, tok), 1)

    def pick(g):
        row = loss_ck[pl.ds(chunk_of(g, 0), 1), :]
        return pltpu.roll(row, lax.rem(2 * ct - mnr[g] * half + g * half, ct), 1)[:, 0:tok]

    loss_out[...] = jnp.where(lane1 < half, pick(0), pick(1))
    loss_send.wait()
    mean_out[...] = (pair[2] + pair[3])[0:1, 0:1] / total_n

    for d in range(1, ndev):
        s = dl_all.at[lax.rem(me + ndev - d, ndev)]
        rcopy(s, s, dl_s.at[d], dl_r.at[d], {"tp": me}).wait_recv()
    dl = jnp.sum(dl_all[...], axis=0)
    for j in range(dim // tok):
        dln_out[0:1, j * tok:(j + 1) * tok] = dl[j:j + 1]
        dln_out[1:2, j * tok:(j + 1) * tok] = dl[4 + j:5 + j]

    for g in PAIR:
        for k in range(4):
            ag1(g, k).wait_send()
            ag2(g, k).wait_send()
        for k in range(6):
            ring1[g].copy(k).wait_send()
            ring2[g].copy(k).wait_send()
    for cp in tms + sts + dls:
        cp.wait_send()
    e_send.wait_send()
    cnt_send.wait_send()
    de_send.wait_send()
    de_out.wait()


def adam_kernel(dE, emb, m1, m2, dln, lnp, lm1, lm2, loss, mean, dh,
                e_new, m1_new, m2_new, ln_new, lm1_new, lm2_new, loss_o, mean_o, dh_o):
    p, a, b = adam_step(emb[...].astype(F32), dE[...], m1[...], m2[...], WEIGHT_DECAY)
    e_new[...] = p.astype(BF16)
    m1_new[...] = a
    m2_new[...] = b

    @pl.when(pl.program_id(0) == 0)
    def _():
        p, a, b = adam_step(lnp[...], dln[...], lm1[...], lm2[...], 0.0)
        ln_new[...] = p
        lm1_new[...] = a
        lm2_new[...] = b
        loss_o[...] = loss[...]
        mean_o[...] = mean[...]
        dh_o[...] = dh[...]


def solution(mesh):
    ntp = mesh.shape["tp"]
    side = math.isqrt(ntp // CORES)
    row_spec = P(("dp", "tp"), None)
    tok_spec = P(("dp", "tp"))
    vocab_spec = P("tp", None)
    repl_spec = P()
    part_spec = P("dp", None)

    def device_step(hidden, targets, loss_mask, ln_params, out_embed, ln_mom1, ln_mom2, embed_mom1, embed_mom2):
        tok, dim = hidden.shape
        voc = out_embed.shape[0]
        half, chips = tok // 2, side * side
        ct, nck = half * side, 2 * side
        ntok = ct * nck
        vpad = -(-voc // 128) * 128
        dma, vm = pltpu.SemaphoreType.DMA, pltpu.VMEM
        dE, dh, dln, loss, mean = pl.pallas_call(
            functools.partial(step_kernel, side),
            out_shape=[jax.ShapeDtypeStruct((voc, dim), F32), jax.ShapeDtypeStruct((tok, dim), BF16),
                       jax.ShapeDtypeStruct((2, dim), F32), jax.ShapeDtypeStruct((1, tok), F32),
                       jax.ShapeDtypeStruct((1, 1), F32)],
            in_specs=[VMEM, VMEM, VMEM, VMEM, ANY],
            out_specs=[ANY, VMEM, VMEM, VMEM, VMEM],
            scratch_shapes=[
                vm((ntok, dim), BF16),
                vm((2, voc, dim), BF16),
                vm((2, dim, vpad), BF16),
                vm((nck // 2, 2, voc, 2 * ct), F32),
                vm((2, vpad, ntok), BF16),
                vm((nck, dim, ct), F32),
                vm((2, 2, dim // 2, ct), F32),
                vm((2, 4, dim // 2, ct), F32),
                vm((2, ct, dim), F32),
                vm((2, 2, half // 2, dim), F32),
                vm((2, 4, half // 2, dim), F32),
                vm((chips, 8, tok), jnp.int32),
                vm((chips, 3, nck, ct), F32),
                *[vm((nck, ct), jnp.int32)] * 2, vm((2, nck, ct), jnp.int32),
                *[vm((nck, ct), F32)] * 3,
                vm((4, 8, tok), F32),
                vm((ntp, 8, tok), F32),
                vm((tok, dim), F32),
                dma((2,)), *[dma((2, 2, 4))] * 2, dma((chips,)), dma((chips,)), dma((chips,)), dma((chips,)),
                *[dma((2, 2, 6))] * 2, dma((ntp,)), dma((ntp,)), *[dma((4,))] * 2,
                pltpu.SemaphoreType.REGULAR,
            ],
            compiler_params=pltpu.CompilerParams(collective_id=0, has_side_effects=True, vmem_limit_bytes=67043328),
            name="head_step",
        )(hidden, targets.reshape(1, tok), loss_mask.reshape(1, tok), ln_params, out_embed)

        blk = 264
        big = pl.BlockSpec((blk, dim), lambda i: (i, 0))

        def whole(s):
            return pl.BlockSpec(s, lambda i: (0, 0))

        small = [whole((2, dim))] * 3
        rest = [whole((1, tok)), whole((1, 1)), whole((tok, dim))]
        e_new, m1n, m2n, lnn, lm1n, lm2n, loss, mean, dh = pl.pallas_call(
            adam_kernel,
            grid=(pl.cdiv(voc, blk),),
            out_shape=[jax.ShapeDtypeStruct((voc, dim), BF16)] + [jax.ShapeDtypeStruct((voc, dim), F32)] * 2
            + [jax.ShapeDtypeStruct((2, dim), F32)] * 3
            + [jax.ShapeDtypeStruct((1, tok), F32), jax.ShapeDtypeStruct((1, 1), F32), jax.ShapeDtypeStruct((tok, dim), BF16)],
            in_specs=[big] * 4 + [whole((2, dim))] + small + rest,
            out_specs=[big] * 3 + small + rest,
            compiler_params=pltpu.CompilerParams(dimension_semantics=("arbitrary",)),
            name="adam_step",
        )(dE, out_embed, embed_mom1, embed_mom2, dln, ln_params, ln_mom1, ln_mom2, loss, mean, dh)
        return (loss.reshape(tok), mean.reshape(1), dh, lnn, lm1n, lm2n, e_new, m1n, m2n)

    return jax.shard_map(device_step, mesh=mesh, in_specs=(row_spec, tok_spec, tok_spec, repl_spec, vocab_spec, repl_spec, repl_spec, vocab_spec, vocab_spec), out_specs=(tok_spec, P("dp"), row_spec, part_spec, part_spec, part_spec, row_spec, row_spec, row_spec), check_vma=False)
```

```python
import functools
import math

import jax
import jax.numpy as jnp
from jax import lax
from jax.experimental import pallas as pl
from jax.experimental.pallas import tpu as pltpu
from jax.sharding import PartitionSpec as P

LN_EPS = 1e-5
BETA_ONE = 0.9
BETA_TWO = 0.95
ADAM_EPS = 1e-8
LEARN_RATE = 1e-3
WEIGHT_DECAY = 0.1
ADAM_STEP = 10
MESH = pl.DeviceIdType.MESH
CORES = 2
PAIR = (0, 1)
TILE = 528
ANY = pl.BlockSpec(memory_space=pl.ANY)
F32, BF16 = jnp.float32, jnp.bfloat16
NN = (((1,), (0,)), ((), ()))
NT = (((1,), (1,)), ((), ()))


def adam_step(param_val, grad_val, m_old, v_old, decay_rate):
    m_new = BETA_ONE * m_old + (1.0 - BETA_ONE) * grad_val
    v_new = BETA_TWO * v_old + (1.0 - BETA_TWO) * grad_val * grad_val
    m_hat = m_new / (1.0 - BETA_ONE ** ADAM_STEP)
    v_hat = v_new / (1.0 - BETA_TWO ** ADAM_STEP)
    new_param = param_val - LEARN_RATE * (m_hat / (jnp.sqrt(v_hat) + ADAM_EPS) + decay_rate * param_val)
    return new_param, m_new, v_new


def row_tiles(rows, size):
    return [(r, min(size, rows - r)) for r in range(0, rows, size)]


def step_kernel(side, hid_hbm, tgt_hbm, msk_hbm, lnp_hbm, emb_ref,
                dE_out, dh_out, dln_out, sm_out,
                hid_ref, tgt_ref, msk_ref, lnp_ref, dh_buf, dln_buf, sm_buf,
                xg, ee, et, ez, dz, dxp, r1, r2, q1, q2,
                tm_all, st_all, tl_all, tgt_ck, msk_ck, rel_ck, top_ck, lse_ck, s_ck, loss_ck, pair, dl_all,
                in_sem, out_sem, ag1_s, ag1_r, ag2_s, ag2_r, ag3_s, ag3_r, tm_s, tm_r, st_s, st_r, tl_s, tl_r,
                rs_s, rs_r, ring_s, ring_r, dl_s, dl_r, pr_s, pr_r, free_sem):
    chips = side * side
    ndev = chips * CORES
    tok, dim = hid_ref.shape
    half = tok // 2
    voc = emb_ref.shape[0]
    pairs = side // 2
    ct = 2 * tok
    nck = side * pairs
    hd, qd = dim // 2, dim // 4
    plus, minus = 1, side - 1
    me = lax.axis_index("tp")
    core = lax.rem(me, CORES)
    chip = me // CORES
    mx, my = lax.rem(chip, side), chip // side
    odd = lax.rem(mx, 2)
    sib = me + 1 - 2 * core

    def chip_at(dy, dx):
        return lax.rem(my + dy, side) * side + lax.rem(mx + dx, side)

    def rel(g, dmaj, dmin):
        return (dmin, dmaj) if g else (dmaj, dmin)

    def dev(g, dmaj, dmin):
        return {"tp": chip_at(*rel(g, dmaj, dmin)) * CORES + core}

    def rcopy(src, dst, ssem, rsem, device):
        return pltpu.make_async_remote_copy(src_ref=src, dst_ref=dst, send_sem=ssem, recv_sem=rsem,
                                            device_id=device, device_id_type=MESH)

    loads = [pltpu.make_async_copy(s, d, in_sem.at[i]) for i, (s, d) in enumerate(
        ((hid_hbm, hid_ref), (lnp_hbm, lnp_ref), (tgt_hbm, tgt_ref), (msk_hbm, msk_ref), (emb_ref, ee.at[0])))]
    for cp in loads:
        cp.start()
    barrier = pltpu.get_barrier_semaphore()
    for d in range(1, ndev):
        pl.semaphore_signal(barrier, inc=1, device_id={"tp": lax.rem(me + d, ndev)}, device_id_type=MESH)
    for cp in loads[:4]:
        cp.wait()

    def normalize():
        rows = hid_ref[...].astype(F32)
        cent = rows - jnp.mean(rows, axis=-1, keepdims=True)
        rstd = lax.rsqrt(jnp.mean(cent * cent, axis=-1, keepdims=True) + LN_EPS)
        return cent * rstd, rstd

    xb = (normalize()[0] * lnp_ref[0:1, :] + lnp_ref[1:2, :]).astype(BF16)

    def xslot(g, dmaj, dmin, r0=0, n=half):
        row = chip_at(*rel(g, dmaj, dmin)) * tok + g * half + r0
        return xg.at[pl.ds(pl.multiple_of(row, 32), n)]

    xg[pl.ds(pl.multiple_of(chip * tok, tok), tok), :] = xb
    tm_all[chip, 0:1, :] = tgt_ref[...]
    tm_all[chip, 1:2, :] = msk_ref[...]
    et[:, :, voc:] = jnp.zeros((2, dim, et.shape[2] - voc), BF16)
    dz[:, voc:, :] = jnp.zeros((2, dz.shape[1] - voc, dz.shape[2]), BF16)

    pl.semaphore_wait(barrier, ndev - 1)

    ways = (plus, minus)
    back = (minus, plus)

    def first(g, k, dmin=0):
        s = xslot(g, 0, dmin)
        return rcopy(s, s, ag1_s.at[g, 0, k], ag1_r.at[g, 0, k], dev(g, 0, ways[k]))

    def first_fwd(g, k, dmin):
        s = xslot(g, 0, dmin, k * (half // 2), half // 2)
        return rcopy(s, s, ag1_s.at[g, 1, k], ag1_r.at[g, 1, k], dev(g, 0, ways[k]))

    rel_pos = (0, minus, plus, 2)

    def second(g, r, k, dmaj=0):
        s = xslot(g, dmaj, rel_pos[r])
        return rcopy(s, s, ag2_s.at[g, r, k], ag2_r.at[g, r, k], dev(g, ways[k], 0))

    def third(g, r, dmaj):
        s = xslot(g, dmaj, rel_pos[r])
        return rcopy(s, s, ag3_s.at[g, r], ag3_r.at[g, r], dev(g, ways[r // 2], 0))

    def to_peers(ref, ssem, rsem):
        out = []
        for d in range(1, chips):
            out.append(rcopy(ref, ref, ssem.at[d], rsem.at[d], {"tp": lax.rem(chip + d, chips) * CORES + core}))
            out[-1].start()
        return out

    def from_peers(ref_of, ssem, rsem):
        for d in range(1, chips):
            s = ref_of(lax.rem(chip + chips - d, chips))
            rcopy(s, s, ssem.at[d], rsem.at[d], {"tp": sib}).wait_recv()

    tms = to_peers(tm_all.at[chip], tm_s, tm_r)
    for g in PAIR:
        for k in PAIR:
            first(g, k).start()
    e_send = rcopy(emb_ref, ee.at[1], pr_s.at[0], pr_r.at[0], {"tp": sib})
    e_send.start()
    for g in PAIR:
        for k in PAIR:
            second(g, 0, k).start()

    for k in PAIR:
        for g in PAIR:
            first(g, k, back[k]).wait_recv()
            first_fwd(g, k, back[k]).start()
    for k in PAIR:
        for g in PAIR:
            for j in PAIR:
                second(g, 1 + k, j).start()

    def transpose_e(h):
        for r0, n in row_tiles(voc, 384):
            et[h, :, r0:r0 + n] = ee[h, r0:r0 + n, :].T

    loads[-1].wait()
    transpose_e(0)
    for g in PAIR:
        for k in PAIR:
            second(g, 0, k, back[k]).wait_recv()
        third(g, 0, minus).start()
    from_peers(lambda t: tm_all.at[t], tm_s, tm_r)
    for c in range(nck):
        for j in PAIR:
            v = tm_all[2 * c + j]
            tgt_ck[c:c + 1, j * tok:(j + 1) * tok] = v[0:1]
            msk_ck[c:c + 1, j * tok:(j + 1) * tok] = v[1:2]
    rel_ck[0] = tgt_ck[...] - me * voc
    rel_ck[1] = tgt_ck[...] - sib * voc
    maskf = msk_ck[...].astype(F32)
    pair[0] = jnp.broadcast_to(jnp.sum(maskf, keepdims=True), (8, tok))
    cnt_send = rcopy(pair.at[0], pair.at[1], pr_s.at[1], pr_r.at[1], {"tp": sib})
    cnt_send.start()
    e_send.wait_recv()
    transpose_e(1)

    tiles = [(h, r0, n) for h in PAIR for r0, n in row_tiles(voc, TILE)]

    def chunk_at(dy, dj):
        y, j = lax.rem(my + dy, side), lax.rem(mx // 2 + dj, pairs)
        return y * pairs + j, y, pl.multiple_of(j * ct, ct)

    def logits_chunk(dy, dj):
        c, i, lane0 = chunk_at(dy, dj)
        x_c = xg[pl.ds(pl.multiple_of(c * ct, ct), ct), :]
        top = None
        for h, r0, n in tiles:
            z = lax.dot_general(ee[h, r0:r0 + n, :], x_c, NT, preferred_element_type=F32)
            ez[i, h, r0:r0 + n, pl.ds(lane0, ct)] = z
            t = jnp.max(z, axis=0, keepdims=True)
            top = t if top is None else jnp.maximum(top, t)
        tot = jnp.zeros((1, ct), F32)
        tl = jnp.zeros((1, ct), F32)
        for h, r0, n in tiles:
            z = ez[i, h, r0:r0 + n, pl.ds(lane0, ct)]
            e = jnp.exp(z - top)
            ez[i, h, r0:r0 + n, pl.ds(lane0, ct)] = e
            tot += jnp.sum(e, axis=0, keepdims=True)
            hit = lax.broadcasted_iota(jnp.int32, (n, ct), 0) == rel_ck[h, pl.ds(c, 1), :] - r0
            tl += jnp.sum(jnp.where(hit, z, 0.0), axis=0, keepdims=True)
        top_ck[pl.ds(c, 1), :] = top
        tl_all[chip, pl.ds(c, 1), :] = tl
        st_all[c, chip] = top + jnp.log(tot)
        to_peers(st_all.at[c, chip], st_s.at[c], st_r.at[c])

    def gather1():
        for g in PAIR:
            for r in (1, 2):
                for k in PAIR:
                    second(g, r, k, back[k]).wait_recv()
                third(g, r, back[r // 2]).start()
        for g in PAIR:
            for k in PAIR:
                first_fwd(g, k, 2).wait_recv()
            for j in PAIR:
                second(g, 3, j).start()

    def gather3():
        for g in PAIR:
            third(g, 0, 2).wait_recv()

    def gather4():
        for g in PAIR:
            for k in PAIR:
                second(g, 3, k, back[k]).wait_recv()
            third(g, 3, plus).start()
        for g in PAIR:
            for r in (1, 2):
                third(g, r, 2).wait_recv()

    def gather7():
        for g in PAIR:
            third(g, 3, 2).wait_recv()

    def logits_step(k, carry):
        for i, event in ((1, gather1), (3, gather3), (4, gather4), (7, gather7)):
            pl.when(k == i)(event)
        far, t = k // 6, lax.rem(k, 3)
        logits_chunk((t + t // 2) * (1 - far) + 2 * far, (k // 3) * (1 - far) + (k - 6) * far)
        return carry

    lax.fori_loop(0, nck, logits_step, 0)
    tls = to_peers(tl_all.at[chip], tl_s, tl_r)
    cnt_send.wait_recv()
    total_n = (pair[0] + pair[1])[0:1, 0:1]
    s_ck[...] = maskf / total_n

    def grad_chunk(dy, dj):
        c, i, lane0 = chunk_at(dy, dj)
        out0 = pl.multiple_of(c * ct, ct)
        from_peers(lambda t: st_all.at[c, t], st_s.at[c], st_r.at[c])
        part = st_all[c]
        top = jnp.max(part, axis=0)
        lse = top + jnp.log(jnp.sum(jnp.exp(part - top[None]), axis=0))
        lse_ck[pl.ds(c, 1), :] = lse
        s = s_ck[pl.ds(c, 1), :]
        a = jnp.exp(top_ck[pl.ds(c, 1), :] - lse) * s
        for h, r0, n in tiles:
            e = ez[i, h, r0:r0 + n, pl.ds(lane0, ct)]
            hit = lax.broadcasted_iota(jnp.int32, (n, ct), 0) == rel_ck[h, pl.ds(c, 1), :] - r0
            dz[h, r0:r0 + n, pl.ds(out0, ct)] = (e * a - jnp.where(hit, s, 0.0)).astype(BF16)
        for q in PAIR:
            acc = None
            for h in PAIR:
                t = lax.dot_general(et[h, q * hd:(q + 1) * hd, :], dz[h, :, pl.ds(out0, ct)], NN,
                                    preferred_element_type=F32)
                acc = t if acc is None else acc + t
            for j in PAIR:
                dxp[2 * c + j, q * hd:(q + 1) * hd, :] = acc[:, j * tok:(j + 1) * tok]

    hops = ((2, 0, 0, minus), (2, 1, 1, plus), (plus, 0, 1, plus), (minus, 1, 2, minus), (minus, 0, 0, minus), (plus, 1, 3, plus))

    def part(g, dmaj, dmin, q):
        return chip_at(*rel(g, dmaj, dmin)), pl.ds(g * hd + q * qd, qd)

    def ring1(g, s, k, hop=None):
        d, q, slot, to = hop or hops[k]
        src = dxp.at[chip_at(*rel(g, d, s)), pl.ds(g * hd + q * qd, qd)]
        land = r2 if hop or k > 1 else r1
        return rcopy(src, land.at[g, s, slot], rs_s.at[g, s, k], rs_r.at[g, s, k], dev(g, to, 0))

    def direct1(g, s, b):
        ring1(g, s, 2 + b, (1 + 2 * b, b, 1 + b, 1 + 2 * b)).start()

    def relay1(g, s):
        for k in PAIR:
            ring1(g, s, k).wait_recv()
            i, q = part(g, ways[1 - k], s, k)
            dxp[i, q, :] = dxp[i, q, :] + r1[g, s, k]
            ring1(g, s, k + 4).start()

    def ring2(g, k):
        d, q, slot, to = hops[k]
        src = dxp.at[chip_at(*rel(g, 0, d)), pl.ds(g * hd + q * qd, qd)]
        return rcopy(src, (q1 if k < 2 else q2).at[g, slot], ring_s.at[g, k], ring_r.at[g, k], dev(g, 0, to))

    def finish1(s):
        for g in PAIR:
            for k in range(2, 6):
                ring1(g, s, k).wait_recv()
            for q in PAIR:
                i, rows = part(g, 0, s, q)
                dxp[i, rows, :] = dxp[i, rows, :] + r2[g, s, 2 * q] + r2[g, s, 2 * q + 1]
            for k in {2: PAIR, plus: (2,), minus: (3,), 0: ()}[s]:
                ring2(g, k).start()

    def relay2():
        for k in PAIR:
            for g in PAIR:
                ring2(g, k).wait_recv()
                i, q = part(g, 0, ways[1 - k], k)
                dxp[i, q, :] = dxp[i, q, :] + q1[g, k]
                ring2(g, k + 4).start()

    near, far = 1 + 2 * odd, 3 - 2 * odd

    def grad_step(dy, dj):
        grad_chunk(dy, dj)
        for s in (2, far) if dj else (0, near):
            for k in {2: PAIR, plus: (2,), minus: (3,), 0: ()}[dy]:
                ring1(0, s, k).start()
        if dj:
            for k in PAIR:
                ring1(1, dy, k).start()
        direct1(1, dy, 1 - odd if dj else odd)

    grad_step(2, 1)
    grad_step(2, 0)
    grad_step(plus, 1)
    grad_step(minus, 1)
    relay1(0, 2)
    relay1(0, far)
    relay1(1, 2)
    grad_step(0, 1)
    grad_step(plus, 0)
    grad_step(minus, 0)
    relay1(0, near)
    relay1(1, plus)
    relay1(1, minus)
    relay1(0, 0)
    grad_step(0, 0)
    relay1(1, 0)
    pl.semaphore_signal(free_sem, inc=1, device_id={"tp": sib}, device_id_type=MESH)

    def embed_grad(h, dst, t):
        r0, n = row_tiles(voc, 528)[t]
        ez[0, dst, r0:r0 + n, :] = lax.dot_general(dz[h, r0:r0 + n, :], xg[...], NN, preferred_element_type=F32)

    for t in range(3):
        embed_grad(1, 0, t)
    pl.semaphore_wait(free_sem, 1)
    de_send = rcopy(ez.at[0, 0], ez.at[1, 0], pr_s.at[3], pr_r.at[3], {"tp": sib})
    de_send.start()

    from_peers(lambda t: tl_all.at[t], tl_s, tl_r)
    loss = (lse_ck[...] - jnp.sum(tl_all[...], axis=0)) * maskf
    loss_ck[...] = loss
    pair[2] = jnp.broadcast_to(jnp.sum(loss, keepdims=True), (8, tok))
    loss_send = rcopy(pair.at[2], pair.at[3], pr_s.at[2], pr_r.at[2], {"tp": sib})
    loss_send.start()

    finish1(2)
    embed_grad(0, 1, 0)
    finish1(plus)
    finish1(minus)
    embed_grad(0, 1, 1)
    relay2()
    finish1(0)
    embed_grad(0, 1, 2)
    de_send.wait_recv()
    for r0, n in row_tiles(voc, 528):
        ez[0, 1, r0:r0 + n, :] = ez[0, 1, r0:r0 + n, :] + ez[1, 0, r0:r0 + n, :]
    de_out = pltpu.make_async_copy(ez.at[0, 1], dE_out, out_sem.at[0])
    de_out.start()
    loss_send.wait_recv()
    sm_buf[...] = (pair[2] + pair[3]) / total_n
    row = loss_ck[pl.ds(chip // 2, 1), :]
    sm_buf[0:1, :] = jnp.where(odd == 0, row[:, :tok], row[:, tok:])
    sm_copy = pltpu.make_async_copy(sm_buf, sm_out, out_sem.at[1])
    sm_copy.start()

    for g in PAIR:
        for k in range(2, 6):
            ring2(g, k).wait_recv()

    own = [dxp[chip, (2 * g + q) * qd:(2 * g + q + 1) * qd, :] + q2[g, 2 * q] + q2[g, 2 * q + 1] for g in PAIR for q in PAIR]
    dx = jnp.concatenate([v.T for v in own], axis=1)
    normed, rstd = normalize()
    dgam = jnp.sum(dx * normed, axis=0, keepdims=True)
    dbet = jnp.sum(dx, axis=0, keepdims=True)
    quarter = dim // tok
    for j in range(quarter):
        dl_all[me, j:j + 1, :] = dgam[:, j * tok:(j + 1) * tok]
        dl_all[me, quarter + j:quarter + j + 1, :] = dbet[:, j * tok:(j + 1) * tok]
    dls = []
    for d in range(1, ndev):
        cp = rcopy(dl_all.at[me], dl_all.at[me], dl_s.at[d], dl_r.at[d], {"tp": lax.rem(me + d, ndev)})
        cp.start()
        dls.append(cp)
    dn = dx * lnp_ref[0:1, :]
    dh = rstd * (dn - jnp.mean(dn, axis=-1, keepdims=True) - normed * jnp.mean(dn * normed, axis=-1, keepdims=True))
    dh_buf[...] = dh.astype(BF16)
    dh_copy = pltpu.make_async_copy(dh_buf, dh_out, out_sem.at[2])
    dh_copy.start()

    for g in PAIR:
        for k in PAIR:
            first(g, k).wait_send()
            first_fwd(g, k, back[k]).wait_send()
        for r in range(4):
            for k in PAIR:
                second(g, r, k).wait_send()
            third(g, r, back[r // 2]).wait_send()
        for k in range(6):
            for s in range(side):
                ring1(g, s, k).wait_send()
            ring2(g, k).wait_send()
    for c in range(nck):
        for d in range(1, chips):
            rcopy(st_all.at[c, chip], st_all.at[c, chip], st_s.at[c, d], st_r.at[c, d], {"tp": sib}).wait_send()
    for cp in tms + tls + [e_send, cnt_send, de_send, loss_send]:
        cp.wait_send()

    for d in range(1, ndev):
        s = dl_all.at[lax.rem(me + ndev - d, ndev)]
        rcopy(s, s, dl_s.at[d], dl_r.at[d], {"tp": sib}).wait_recv()
    dl = jnp.sum(dl_all[...], axis=0)
    for j in range(quarter):
        for i in PAIR:
            dln_buf[i:i + 1, j * tok:(j + 1) * tok] = dl[i * quarter + j:i * quarter + j + 1]
    dln_copy = pltpu.make_async_copy(dln_buf, dln_out, out_sem.at[3])
    dln_copy.start()
    for cp in dls:
        cp.wait_send()
    for cp in (de_out, sm_copy, dh_copy, dln_copy):
        cp.wait()


def adam_kernel(*refs):
    big_in, small_in = refs[:4], refs[4:10]
    e_new, m1_new, m2_new, ln_new, lm1_new, lm2_new, loss_o, mean_o, dh_o = refs[10:19]
    scratch = refs[19:]
    big_buf, small_buf, big_res, ln_res, loss_res, mean_res = scratch[:4], scratch[4:10], scratch[10:13], scratch[13:16], scratch[16], scratch[17]
    in_sem, small_sem, out_sem, sout_sem = scratch[18:]
    tiles = row_tiles(big_in[0].shape[0], 272)
    small = [pltpu.make_async_copy(s, d, small_sem.at[i]) for i, (s, d) in enumerate(zip(small_in, small_buf))]
    reads = [[pltpu.make_async_copy(s.at[pl.ds(r0, n)], d.at[pl.ds(r0, n)], in_sem.at[t, i])
              for i, (s, d) in enumerate(zip(big_in, big_buf))] for t, (r0, n) in enumerate(tiles)]
    for cp in reads[0] + small:
        cp.start()
    for row in reads[1:]:
        for cp in row:
            cp.start()
    writes = []
    for t, (r0, n) in enumerate(tiles):
        for cp in reads[t]:
            cp.wait()
        sl = slice(r0, r0 + n)
        grad, emb, m1, m2 = [b[sl, :] for b in big_buf]
        res = adam_step(emb.astype(F32), grad, m1, m2, WEIGHT_DECAY)
        for i, (buf, dst, val) in enumerate(zip(big_res, (e_new, m1_new, m2_new), res)):
            buf[sl, :] = val.astype(buf.dtype)
            writes.append(pltpu.make_async_copy(buf.at[pl.ds(r0, n)], dst.at[pl.ds(r0, n)], out_sem.at[t, i]))
            writes[-1].start()
    for cp in small:
        cp.wait()
    dln, lnp, lm1, lm2, sm, dh = small_buf
    for buf, val in zip(ln_res, adam_step(lnp[...], dln[...], lm1[...], lm2[...], 0.0)):
        buf[...] = val
    loss_res[...] = sm[0:1, :]
    mean_res[...] = sm[1:2, 0:1]
    for i, (src, dst) in enumerate(zip((*ln_res, loss_res, mean_res, dh), (ln_new, lm1_new, lm2_new, loss_o, mean_o, dh_o))):
        writes.append(pltpu.make_async_copy(src, dst, sout_sem.at[i]))
        writes[-1].start()
    for cp in writes:
        cp.wait()


def solution(mesh):
    ntp = mesh.shape["tp"]
    side = math.isqrt(ntp // CORES)
    row_spec = P(("dp", "tp"), None)
    tok_spec = P(("dp", "tp"))
    vocab_spec = P("tp", None)
    repl_spec = P()
    part_spec = P("dp", None)

    def device_step(hidden, targets, loss_mask, ln_params, out_embed, ln_mom1, ln_mom2, embed_mom1, embed_mom2):
        tok, dim = hidden.shape
        voc = out_embed.shape[0]
        half, chips = tok // 2, side * side
        ct, nck, qd = 2 * tok, chips // 2, dim // 4
        ntok = ct * nck
        vpad = -(-voc // 128) * 128
        dma, vm = pltpu.SemaphoreType.DMA, pltpu.VMEM
        big, sem2 = jax.ShapeDtypeStruct((voc, dim), F32), [dma((2, 2, 2))] * 2
        ln_s, sm_s = jax.ShapeDtypeStruct((2, dim), F32), jax.ShapeDtypeStruct((8, tok), F32)
        dh_s = jax.ShapeDtypeStruct((tok, dim), BF16)
        dE, dh, dln, sm = pl.pallas_call(
            functools.partial(step_kernel, side),
            out_shape=[big, dh_s, ln_s, sm_s],
            in_specs=[ANY] * 5,
            out_specs=[ANY] * 4,
            scratch_shapes=[
                vm((tok, dim), BF16), *[vm((1, tok), jnp.int32)] * 2, vm((2, dim), F32),
                vm((tok, dim), BF16), vm((2, dim), F32), vm((8, tok), F32),
                vm((ntok, dim), BF16),
                vm((2, voc, dim), BF16),
                vm((2, dim, vpad), BF16),
                vm((nck // 2, 2, voc, 2 * ct), F32),
                vm((2, vpad, ntok), BF16),
                vm((chips, dim, tok), F32),
                vm((2, side, 2, qd, tok), F32),
                vm((2, side, 4, qd, tok), F32),
                vm((2, 2, qd, tok), F32),
                vm((2, 4, qd, tok), F32),
                vm((chips, 2, tok), jnp.int32),
                vm((nck, chips, 1, ct), F32),
                vm((chips, nck, ct), F32),
                *[vm((nck, ct), jnp.int32)] * 2, vm((2, nck, ct), jnp.int32),
                *[vm((nck, ct), F32)] * 4,
                vm((4, 8, tok), F32),
                vm((ntp, 8, tok), F32),
                dma((5,)), dma((4,)), *sem2, *[dma((2, 4, 2))] * 2, *[dma((2, 4))] * 2,
                *[dma((chips,))] * 2, *[dma((nck, chips))] * 2, *[dma((chips,))] * 2,
                *[dma((2, side, 6))] * 2, *[dma((2, 6))] * 2, *[dma((ntp,))] * 2, *[dma((4,))] * 2,
                pltpu.SemaphoreType.REGULAR,
            ],
            compiler_params=pltpu.CompilerParams(collective_id=0, has_side_effects=True, vmem_limit_bytes=67043328),
            name="head_step",
        )(hidden, targets.reshape(1, tok), loss_mask.reshape(1, tok), ln_params, out_embed)

        big_b, nt = jax.ShapeDtypeStruct((voc, dim), BF16), len(row_tiles(voc, 272))
        shapes = [big, big_b, big, big, ln_s, ln_s, ln_s, ln_s, sm_s, dh_s]
        outs = [big_b, big, big, ln_s, ln_s, ln_s, jax.ShapeDtypeStruct((1, tok), F32), jax.ShapeDtypeStruct((1, 1), F32), dh_s]
        e_new, m1n, m2n, lnn, lm1n, lm2n, loss, mean, dh = pl.pallas_call(
            adam_kernel,
            out_shape=outs,
            in_specs=[ANY] * len(shapes),
            out_specs=[ANY] * len(outs),
            scratch_shapes=[vm(s.shape, s.dtype) for s in shapes + outs[:8]]
            + [dma((nt, 4)), dma((6,)), dma((nt, 3)), dma((6,))],
            compiler_params=pltpu.CompilerParams(vmem_limit_bytes=67043328),
            name="adam_step",
        )(dE, out_embed, embed_mom1, embed_mom2, dln, ln_params, ln_mom1, ln_mom2, sm, dh)
        return (loss.reshape(tok), mean.reshape(1), dh, lnn, lm1n, lm2n, e_new, m1n, m2n)

    return jax.shard_map(device_step, mesh=mesh, in_specs=(row_spec, tok_spec, tok_spec, repl_spec, vocab_spec, repl_spec, repl_spec, vocab_spec, vocab_spec), out_specs=(tok_spec, P("dp"), row_spec, part_spec, part_spec, part_spec, row_spec, row_spec, row_spec), check_vma=False)
```

```python
import functools
import math

import jax
import jax.numpy as jnp
from jax import lax
from jax.experimental import pallas as pl
from jax.experimental.pallas import tpu as pltpu
from jax.sharding import PartitionSpec as P

LN_EPS = 1e-5
BETA_ONE = 0.9
BETA_TWO = 0.95
ADAM_EPS = 1e-8
LEARN_RATE = 1e-3
WEIGHT_DECAY = 0.1
ADAM_STEP = 10
MESH = pl.DeviceIdType.MESH
CORES = 2
PAIR = (0, 1)
TILE = 320
ANY = pl.BlockSpec(memory_space=pl.ANY)
F32, BF16 = jnp.float32, jnp.bfloat16
NN = (((1,), (0,)), ((), ()))
NT = (((1,), (1,)), ((), ()))


def adam_step(param_val, grad_val, m_old, v_old, decay_rate):
    m_new = BETA_ONE * m_old + (1.0 - BETA_ONE) * grad_val
    v_new = BETA_TWO * v_old + (1.0 - BETA_TWO) * grad_val * grad_val
    m_hat = m_new / (1.0 - BETA_ONE ** ADAM_STEP)
    v_hat = v_new / (1.0 - BETA_TWO ** ADAM_STEP)
    new_param = param_val - LEARN_RATE * (m_hat / (jnp.sqrt(v_hat) + ADAM_EPS) + decay_rate * param_val)
    return new_param, m_new, v_new


def row_tiles(rows, size):
    return [(r, min(size, rows - r)) for r in range(0, rows, size)]


def step_kernel(side, hid_hbm, tgt_hbm, msk_hbm, lnp_hbm, emb_ref,
                dE_out, dh_out, dln_out, sm_out,
                hid_ref, tgt_ref, msk_ref, lnp_ref, dh_buf, dln_buf, sm_buf,
                xg, ee, et, ez, dz, dxp, r1, r2, q1, q2,
                tm_all, st_all, tl_all, zb, tgt_ck, msk_ck, rel_ck, top_ck, lse_ck, s_ck, loss_ck, pair, dl_all,
                in_sem, out_sem, ag_s, ag1_r, ag2_r, ag3_r, tm_s, tm_r, st_s, st_r, tl_s, tl_r,
                rs_s, rs_r, ring_r, dl_s, dl_r, pr_s, pr_r, free_sem):
    chips = side * side
    ndev = chips * CORES
    tok, dim = hid_ref.shape
    half = tok // 2
    voc = emb_ref.shape[0]
    pairs = side // 2
    ct = 2 * tok
    nck = side * pairs
    hd, qd = dim // 2, dim // 4
    plus, minus = 1, side - 1
    me = lax.axis_index("tp")
    core = lax.rem(me, CORES)
    chip = me // CORES
    mx, my = lax.rem(chip, side), chip // side
    odd = lax.rem(mx, 2)
    sib = me + 1 - 2 * core

    def chip_at(dy, dx):
        return lax.rem(my + dy, side) * side + lax.rem(mx + dx, side)

    def rel(g, dmaj, dmin):
        return (dmin, dmaj) if g else (dmaj, dmin)

    def dev(g, dmaj, dmin):
        return {"tp": chip_at(*rel(g, dmaj, dmin)) * CORES + core}

    def rcopy(src, dst, ssem, rsem, device):
        return pltpu.make_async_remote_copy(src_ref=src, dst_ref=dst, send_sem=ssem, recv_sem=rsem,
                                            device_id=device, device_id_type=MESH)

    loads = [pltpu.make_async_copy(s, d, in_sem.at[i]) for i, (s, d) in enumerate(
        ((hid_hbm, hid_ref), (lnp_hbm, lnp_ref), (tgt_hbm, tgt_ref), (msk_hbm, msk_ref), (emb_ref, ee.at[0])))]
    for cp in loads:
        cp.start()
    barrier = pltpu.get_barrier_semaphore()
    for d in range(1, ndev):
        pl.semaphore_signal(barrier, inc=1, device_id={"tp": lax.rem(me + d, ndev)}, device_id_type=MESH)
    for cp in loads[:4]:
        cp.wait()

    def normalize():
        rows = hid_ref[...].astype(F32)
        cent = rows - jnp.mean(rows, axis=-1, keepdims=True)
        rstd = lax.rsqrt(jnp.mean(cent * cent, axis=-1, keepdims=True) + LN_EPS)
        return cent * rstd, rstd

    xb = (normalize()[0] * lnp_ref[0:1, :] + lnp_ref[1:2, :]).astype(BF16)

    def xslot(g, dmaj, dmin, r0=0, n=half):
        row = chip_at(*rel(g, dmaj, dmin)) * tok + g * half + r0
        return xg.at[pl.ds(pl.multiple_of(row, 32), n)]

    xg[pl.ds(pl.multiple_of(chip * tok, tok), tok), :] = xb
    tm_all[chip, 0:1, :] = tgt_ref[...]
    tm_all[chip, 1:2, :] = msk_ref[...]
    et[:, :, voc:] = jnp.zeros((2, dim, et.shape[2] - voc), BF16)
    dz[:, voc:, :] = jnp.zeros((2, dz.shape[1] - voc, dz.shape[2]), BF16)

    pl.semaphore_wait(barrier, ndev - 1)

    ways = (plus, minus)
    back = (minus, plus)

    def first(g, k, dmin=0):
        s = xslot(g, 0, dmin)
        return rcopy(s, s, ag_s, ag1_r.at[g, 0, k], dev(g, 0, ways[k]))

    def first_fwd(g, k, dmin):
        s = xslot(g, 0, dmin, k * (half // 2), half // 2)
        return rcopy(s, s, ag_s, ag1_r.at[g, 1, k], dev(g, 0, ways[k]))

    rel_pos = (0, minus, plus, 2)

    def second(g, r, k, dmaj=0):
        s = xslot(g, dmaj, rel_pos[r])
        return rcopy(s, s, ag_s, ag2_r.at[g, r, k], dev(g, ways[k], 0))

    def third(g, r, dmaj):
        s = xslot(g, dmaj, rel_pos[r])
        return rcopy(s, s, ag_s, ag3_r.at[g, r], dev(g, ways[r // 2], 0))

    def to_peers(ref, ssem, rsem):
        for d in range(1, chips):
            rcopy(ref, ref, ssem, rsem, {"tp": lax.rem(chip + d, chips) * CORES + core}).start()

    def all_of(ref, ssem, rsem):
        return rcopy(ref, ref, ssem, rsem, {"tp": sib})

    to_peers(tm_all.at[chip], tm_s, tm_r)
    tms = all_of(tm_all.at[pl.ds(0, chips - 1)], tm_s, tm_r)
    for g in PAIR:
        for k in PAIR:
            first(g, k).start()
    e_send = rcopy(emb_ref, ee.at[1], pr_s.at[0], pr_r.at[0], {"tp": sib})
    e_send.start()
    for g in PAIR:
        for k in PAIR:
            second(g, 0, k).start()

    for k in PAIR:
        for g in PAIR:
            first(g, k, back[k]).wait_recv()
            first_fwd(g, k, back[k]).start()
    for k in PAIR:
        for g in PAIR:
            for j in PAIR:
                second(g, 1 + k, j).start()

    def transpose_e(h):
        for r0, n in row_tiles(voc, 384):
            et[h, :, r0:r0 + n] = ee[h, r0:r0 + n, :].T

    loads[-1].wait()
    transpose_e(0)
    for g in PAIR:
        for k in PAIR:
            second(g, 0, k, back[k]).wait_recv()
        third(g, 0, minus).start()
    tms.wait_recv()
    for c in range(nck):
        for j in PAIR:
            v = tm_all[2 * c + j]
            tgt_ck[c:c + 1, j * tok:(j + 1) * tok] = v[0:1]
            msk_ck[c:c + 1, j * tok:(j + 1) * tok] = v[1:2]
    rel_ck[0] = tgt_ck[...] - me * voc
    rel_ck[1] = tgt_ck[...] - sib * voc
    maskf = msk_ck[...].astype(F32)
    pair[0] = jnp.broadcast_to(jnp.sum(maskf, keepdims=True), (8, tok))
    cnt_send = rcopy(pair.at[0], pair.at[1], pr_s.at[1], pr_r.at[1], {"tp": sib})
    cnt_send.start()
    e_send.wait_recv()
    transpose_e(1)

    tiles = [(h, r0, n) for h in PAIR for r0, n in row_tiles(voc, TILE)]

    def chunk_at(dy, dj):
        y, j = lax.rem(my + dy, side), lax.rem(mx // 2 + dj, pairs)
        return y * pairs + j, y, pl.multiple_of(j * ct, ct)

    def logits_chunk(dy, dj):
        c, i, lane0 = chunk_at(dy, dj)
        x_c = xg[pl.ds(pl.multiple_of(c * ct, ct), ct), :]
        tops, tots = [], []
        tl = jnp.zeros((1, ct), F32)

        def finish_tile(t):
            h, r0, n = tiles[t]
            z = zb[t % 2, :n, :]
            e = jnp.exp(z - tops[t])
            ez[i, h, r0:r0 + n, pl.ds(lane0, ct)] = e
            tots.append(jnp.sum(e, axis=0, keepdims=True))
            hit = lax.broadcasted_iota(jnp.int32, (n, ct), 0) == rel_ck[h, pl.ds(c, 1), :] - r0
            return jnp.sum(jnp.where(hit, z, 0.0), axis=0, keepdims=True)

        for t, (h, r0, n) in enumerate(tiles):
            z = lax.dot_general(ee[h, r0:r0 + n, :], x_c, NT, preferred_element_type=F32)
            zb[t % 2, :n, :] = z
            tops.append(jnp.max(z, axis=0, keepdims=True))
            if t:
                tl += finish_tile(t - 1)
        tl += finish_tile(len(tiles) - 1)
        top = functools.reduce(jnp.maximum, tops)
        tot = sum(s * jnp.exp(m - top) for m, s in zip(tops, tots))
        for t, m in enumerate(tops):
            top_ck[t, pl.ds(c, 1), :] = m
        tl_all[chip, pl.ds(c, 1), :] = tl
        st_all[c, chip] = top + jnp.log(tot)
        to_peers(st_all.at[c, chip], st_s, st_r.at[c])

    def gather1():
        for g in PAIR:
            for r in (1, 2):
                for k in PAIR:
                    second(g, r, k, back[k]).wait_recv()
                third(g, r, back[r // 2]).start()
        for g in PAIR:
            for k in PAIR:
                first_fwd(g, k, 2).wait_recv()
            for j in PAIR:
                second(g, 3, j).start()

    def gather3():
        for g in PAIR:
            third(g, 0, 2).wait_recv()

    def gather4():
        for g in PAIR:
            for k in PAIR:
                second(g, 3, k, back[k]).wait_recv()
            third(g, 3, plus).start()
        for g in PAIR:
            for r in (1, 2):
                third(g, r, 2).wait_recv()

    def gather7():
        for g in PAIR:
            third(g, 3, 2).wait_recv()

    def logits_step(k, carry):
        for i, event in ((1, gather1), (3, gather3), (4, gather4), (7, gather7)):
            pl.when(k == i)(event)
        far, t = k // 6, lax.rem(k, 3)
        logits_chunk((t + t // 2) * (1 - far) + 2 * far, (k // 3) * (1 - far) + (k - 6) * far)
        return carry

    lax.fori_loop(0, nck, logits_step, 0)
    to_peers(tl_all.at[chip], tl_s, tl_r)
    tls = all_of(tl_all.at[pl.ds(0, chips - 1)], tl_s, tl_r)
    cnt_send.wait_recv()
    total_n = (pair[0] + pair[1])[0:1, 0:1]
    s_ck[...] = maskf / total_n

    def grad_chunk(dy, dj):
        c, i, lane0 = chunk_at(dy, dj)
        out0 = pl.multiple_of(c * ct, ct)
        all_of(st_all.at[c, pl.ds(0, chips - 1)], st_s, st_r.at[c]).wait_recv()
        part = st_all[c]
        top = jnp.max(part, axis=0)
        lse = top + jnp.log(jnp.sum(jnp.exp(part - top[None]), axis=0))
        lse_ck[pl.ds(c, 1), :] = lse
        s = s_ck[pl.ds(c, 1), :]
        for t, (h, r0, n) in enumerate(tiles):
            a = jnp.exp(top_ck[t, pl.ds(c, 1), :] - lse) * s
            e = ez[i, h, r0:r0 + n, pl.ds(lane0, ct)]
            hit = lax.broadcasted_iota(jnp.int32, (n, ct), 0) == rel_ck[h, pl.ds(c, 1), :] - r0
            dz[h, r0:r0 + n, pl.ds(out0, ct)] = (e * a - jnp.where(hit, s, 0.0)).astype(BF16)
        for q in PAIR:
            acc = None
            for h in PAIR:
                t = lax.dot_general(et[h, q * hd:(q + 1) * hd, :], dz[h, :, pl.ds(out0, ct)], NN,
                                    preferred_element_type=F32)
                acc = t if acc is None else acc + t
            for j in PAIR:
                dxp[2 * c + j, q * hd:(q + 1) * hd, :] = acc[:, j * tok:(j + 1) * tok]

    hops = ((2, 0, 0, minus), (2, 1, 1, plus), (plus, 0, 1, plus), (minus, 1, 2, minus), (minus, 0, 0, minus), (plus, 1, 3, plus))

    def part(g, dmaj, dmin, q):
        return chip_at(*rel(g, dmaj, dmin)), pl.ds(g * hd + q * qd, qd)

    def ring1(g, s, k, hop=None):
        d, q, slot, to = hop or hops[k]
        src = dxp.at[chip_at(*rel(g, d, s)), pl.ds(g * hd + q * qd, qd)]
        land = r2 if hop or k > 1 else r1
        return rcopy(src, land.at[g, s, slot], rs_s, rs_r.at[g, s, 2 if hop or k > 1 else k], dev(g, to, 0))

    def direct1(g, s, b):
        ring1(g, s, 2 + b, (1 + 2 * b, b, 1 + b, 1 + 2 * b)).start()

    def relay1(g, s):
        for k in PAIR:
            ring1(g, s, k).wait_recv()
            i, q = part(g, ways[1 - k], s, k)
            dxp[i, q, :] = dxp[i, q, :] + r1[g, s, k]
            ring1(g, s, k + 4).start()

    def ring2(g, k):
        d, q, slot, to = hops[k]
        src = dxp.at[chip_at(*rel(g, 0, d)), pl.ds(g * hd + q * qd, qd)]
        return rcopy(src, (q1 if k < 2 else q2).at[g, slot], rs_s, ring_r.at[g, min(k, 2)], dev(g, 0, to))

    def finish1(s):
        for g in PAIR:
            all_of(r2.at[g, s], rs_s, rs_r.at[g, s, 2]).wait_recv()
            for q in PAIR:
                i, rows = part(g, 0, s, q)
                dxp[i, rows, :] = dxp[i, rows, :] + r2[g, s, 2 * q] + r2[g, s, 2 * q + 1]
            for k in {2: PAIR, plus: (2,), minus: (3,), 0: ()}[s]:
                ring2(g, k).start()

    def relay2():
        for k in PAIR:
            for g in PAIR:
                ring2(g, k).wait_recv()
                i, q = part(g, 0, ways[1 - k], k)
                dxp[i, q, :] = dxp[i, q, :] + q1[g, k]
                ring2(g, k + 4).start()

    near, far = 1 + 2 * odd, 3 - 2 * odd

    def grad_step(dy, dj):
        grad_chunk(dy, dj)
        for s in (2, far) if dj else (0, near):
            for k in {2: PAIR, plus: (2,), minus: (3,), 0: ()}[dy]:
                ring1(0, s, k).start()
        if dj:
            for k in PAIR:
                ring1(1, dy, k).start()
        direct1(1, dy, 1 - odd if dj else odd)

    grad_step(2, 1)
    grad_step(2, 0)
    grad_step(plus, 1)
    grad_step(minus, 1)
    relay1(0, 2)
    relay1(0, far)
    relay1(1, 2)
    grad_step(0, 1)
    grad_step(plus, 0)
    grad_step(minus, 0)
    relay1(0, near)
    relay1(1, plus)
    relay1(1, minus)
    relay1(0, 0)
    grad_step(0, 0)
    relay1(1, 0)
    pl.semaphore_signal(free_sem, inc=1, device_id={"tp": sib}, device_id_type=MESH)

    def embed_grad(h, dst, t):
        r0, n = row_tiles(voc, 528)[t]
        ez[0, dst, r0:r0 + n, :] = lax.dot_general(dz[h, r0:r0 + n, :], xg[...], NN, preferred_element_type=F32)

    for t in range(3):
        embed_grad(1, 0, t)
    pl.semaphore_wait(free_sem, 1)
    de_send = rcopy(ez.at[0, 0], ez.at[1, 0], pr_s.at[3], pr_r.at[3], {"tp": sib})
    de_send.start()

    tls.wait_recv()
    loss = (lse_ck[...] - jnp.sum(tl_all[...], axis=0)) * maskf
    loss_ck[...] = loss
    pair[2] = jnp.broadcast_to(jnp.sum(loss, keepdims=True), (8, tok))
    loss_send = rcopy(pair.at[2], pair.at[3], pr_s.at[2], pr_r.at[2], {"tp": sib})
    loss_send.start()

    finish1(2)
    embed_grad(0, 1, 0)
    finish1(plus)
    finish1(minus)
    embed_grad(0, 1, 1)
    relay2()
    finish1(0)
    embed_grad(0, 1, 2)
    de_send.wait_recv()
    for r0, n in row_tiles(voc, 528):
        ez[0, 1, r0:r0 + n, :] = ez[0, 1, r0:r0 + n, :] + ez[1, 0, r0:r0 + n, :]
    de_out = pltpu.make_async_copy(ez.at[0, 1], dE_out, out_sem.at[0])
    de_out.start()
    loss_send.wait_recv()
    sm_buf[...] = (pair[2] + pair[3]) / total_n
    row = loss_ck[pl.ds(chip // 2, 1), :]
    sm_buf[0:1, :] = jnp.where(odd == 0, row[:, :tok], row[:, tok:])
    sm_copy = pltpu.make_async_copy(sm_buf, sm_out, out_sem.at[1])
    sm_copy.start()

    for g in PAIR:
        all_of(q2.at[g], rs_s, ring_r.at[g, 2]).wait_recv()

    own = [dxp[chip, (2 * g + q) * qd:(2 * g + q + 1) * qd, :] + q2[g, 2 * q] + q2[g, 2 * q + 1] for g in PAIR for q in PAIR]
    dx = jnp.concatenate([v.T for v in own], axis=1)
    normed, rstd = normalize()
    dgam = jnp.sum(dx * normed, axis=0, keepdims=True)
    dbet = jnp.sum(dx, axis=0, keepdims=True)
    quarter = dim // tok
    for j in range(quarter):
        dl_all[me, j:j + 1, :] = dgam[:, j * tok:(j + 1) * tok]
        dl_all[me, quarter + j:quarter + j + 1, :] = dbet[:, j * tok:(j + 1) * tok]
    for d in range(1, ndev):
        rcopy(dl_all.at[me], dl_all.at[me], dl_s, dl_r, {"tp": lax.rem(me + d, ndev)}).start()
    dls = all_of(dl_all.at[pl.ds(0, ndev - 1)], dl_s, dl_r)
    dn = dx * lnp_ref[0:1, :]
    dh = rstd * (dn - jnp.mean(dn, axis=-1, keepdims=True) - normed * jnp.mean(dn * normed, axis=-1, keepdims=True))
    dh_buf[...] = dh.astype(BF16)
    dh_copy = pltpu.make_async_copy(dh_buf, dh_out, out_sem.at[2])
    dh_copy.start()

    blocks = 6 + 16 + 8
    all_of(xg.at[pl.ds(0, blocks * half)], ag_s, pr_r.at[0]).wait_send()
    all_of(dxp.at[pl.ds(0, 12 + 3)], rs_s, pr_r.at[0]).wait_send()
    all_of(st_all.at[:, pl.ds(0, chips - 1)], st_s, pr_r.at[0]).wait_send()
    for cp in (tms, tls, e_send, cnt_send, de_send, loss_send):
        cp.wait_send()

    dls.wait_recv()
    dl = jnp.sum(dl_all[...], axis=0)
    for j in range(quarter):
        for i in PAIR:
            dln_buf[i:i + 1, j * tok:(j + 1) * tok] = dl[i * quarter + j:i * quarter + j + 1]
    dln_copy = pltpu.make_async_copy(dln_buf, dln_out, out_sem.at[3])
    dln_copy.start()
    dls.wait_send()
    for cp in (de_out, sm_copy, dh_copy, dln_copy):
        cp.wait()


def adam_kernel(*refs):
    big_in, small_in = refs[:4], refs[4:10]
    e_new, m1_new, m2_new, ln_new, lm1_new, lm2_new, loss_o, mean_o, dh_o = refs[10:19]
    scratch = refs[19:]
    big_buf, small_buf, big_res, ln_res, loss_res, mean_res = scratch[:4], scratch[4:10], scratch[10:13], scratch[13:16], scratch[16], scratch[17]
    in_sem, small_sem, out_sem, sout_sem = scratch[18:]
    tiles = row_tiles(big_in[0].shape[0], 272)
    small = [pltpu.make_async_copy(s, d, small_sem.at[i]) for i, (s, d) in enumerate(zip(small_in, small_buf))]
    reads = [[pltpu.make_async_copy(s.at[pl.ds(r0, n)], d.at[pl.ds(r0, n)], in_sem.at[t, i])
              for i, (s, d) in enumerate(zip(big_in, big_buf))] for t, (r0, n) in enumerate(tiles)]
    for cp in reads[0] + small:
        cp.start()
    for row in reads[1:]:
        for cp in row:
            cp.start()
    writes = []
    for t, (r0, n) in enumerate(tiles):
        for cp in reads[t]:
            cp.wait()
        sl = slice(r0, r0 + n)
        grad, emb, m1, m2 = [b[sl, :] for b in big_buf]
        res = adam_step(emb.astype(F32), grad, m1, m2, WEIGHT_DECAY)
        for i, (buf, dst, val) in enumerate(zip(big_res, (e_new, m1_new, m2_new), res)):
            buf[sl, :] = val.astype(buf.dtype)
            writes.append(pltpu.make_async_copy(buf.at[pl.ds(r0, n)], dst.at[pl.ds(r0, n)], out_sem.at[i]))
            writes[-1].start()
    for cp in small:
        cp.wait()
    dln, lnp, lm1, lm2, sm, dh = small_buf
    for buf, val in zip(ln_res, adam_step(lnp[...], dln[...], lm1[...], lm2[...], 0.0)):
        buf[...] = val
    loss_res[...] = sm[0:1, :]
    mean_res[...] = sm[1:2, 0:1]
    for i, (src, dst) in enumerate(zip((*ln_res, loss_res, mean_res, dh), (ln_new, lm1_new, lm2_new, loss_o, mean_o, dh_o))):
        writes.append(pltpu.make_async_copy(src, dst, sout_sem.at[i]))
        writes[-1].start()
    for i, buf in enumerate(big_res):
        pltpu.make_async_copy(buf, (e_new, m1_new, m2_new)[i], out_sem.at[i]).wait()
    for cp in writes[-6:]:
        cp.wait()


def solution(mesh):
    ntp = mesh.shape["tp"]
    side = math.isqrt(ntp // CORES)
    row_spec = P(("dp", "tp"), None)
    tok_spec = P(("dp", "tp"))
    vocab_spec = P("tp", None)
    repl_spec = P()
    part_spec = P("dp", None)

    def device_step(hidden, targets, loss_mask, ln_params, out_embed, ln_mom1, ln_mom2, embed_mom1, embed_mom2):
        tok, dim = hidden.shape
        voc = out_embed.shape[0]
        half, chips = tok // 2, side * side
        ct, nck, qd = 2 * tok, chips // 2, dim // 4
        ntok = ct * nck
        vpad = -(-voc // 128) * 128
        dma, vm = pltpu.SemaphoreType.DMA, pltpu.VMEM
        big = jax.ShapeDtypeStruct((voc, dim), F32)
        ln_s, sm_s = jax.ShapeDtypeStruct((2, dim), F32), jax.ShapeDtypeStruct((8, tok), F32)
        dh_s = jax.ShapeDtypeStruct((tok, dim), BF16)
        dE, dh, dln, sm = pl.pallas_call(
            functools.partial(step_kernel, side),
            out_shape=[big, dh_s, ln_s, sm_s],
            in_specs=[ANY] * 5,
            out_specs=[ANY] * 4,
            scratch_shapes=[
                vm((tok, dim), BF16), *[vm((1, tok), jnp.int32)] * 2, vm((2, dim), F32),
                vm((tok, dim), BF16), vm((2, dim), F32), vm((8, tok), F32),
                vm((ntok, dim), BF16),
                vm((2, voc, dim), BF16),
                vm((2, dim, vpad), BF16),
                vm((nck // 2, 2, voc, 2 * ct), F32),
                vm((2, vpad, ntok), BF16),
                vm((chips, dim, tok), F32),
                vm((2, side, 2, qd, tok), F32),
                vm((2, side, 4, qd, tok), F32),
                vm((2, 2, qd, tok), F32),
                vm((2, 4, qd, tok), F32),
                vm((chips, 2, tok), jnp.int32),
                vm((nck, chips, 1, ct), F32),
                vm((chips, nck, ct), F32),
                vm((2, TILE, ct), F32), *[vm((nck, ct), jnp.int32)] * 2, vm((2, nck, ct), jnp.int32),
                vm((2 * len(row_tiles(voc, TILE)), nck, ct), F32), *[vm((nck, ct), F32)] * 3,
                vm((4, 8, tok), F32),
                vm((ntp, 8, tok), F32),
                dma((5,)), dma((4,)), dma(()), dma((2, 2, 2)), dma((2, 4, 2)), dma((2, 4)),
                dma(()), dma(()), dma(()), dma((nck,)), dma(()), dma(()),
                dma(()), dma((2, side, 3)), dma((2, 3)), dma(()), dma(()), *[dma((4,))] * 2,
                pltpu.SemaphoreType.REGULAR,
            ],
            compiler_params=pltpu.CompilerParams(collective_id=0, has_side_effects=True, vmem_limit_bytes=67043328),
            name="head_step",
        )(hidden, targets.reshape(1, tok), loss_mask.reshape(1, tok), ln_params, out_embed)

        big_b, nt = jax.ShapeDtypeStruct((voc, dim), BF16), len(row_tiles(voc, 272))
        shapes = [big, big_b, big, big, ln_s, ln_s, ln_s, ln_s, sm_s, dh_s]
        outs = [big_b, big, big, ln_s, ln_s, ln_s, jax.ShapeDtypeStruct((1, tok), F32), jax.ShapeDtypeStruct((1, 1), F32), dh_s]
        e_new, m1n, m2n, lnn, lm1n, lm2n, loss, mean, dh = pl.pallas_call(
            adam_kernel,
            out_shape=outs,
            in_specs=[ANY] * len(shapes),
            out_specs=[ANY] * len(outs),
            scratch_shapes=[vm(s.shape, s.dtype) for s in shapes + outs[:8]]
            + [dma((nt, 4)), dma((6,)), dma((3,)), dma((6,))],
            compiler_params=pltpu.CompilerParams(vmem_limit_bytes=67043328),
            name="adam_step",
        )(dE, out_embed, embed_mom1, embed_mom2, dln, ln_params, ln_mom1, ln_mom2, sm, dh)
        return (loss.reshape(tok), mean.reshape(1), dh, lnn, lm1n, lm2n, e_new, m1n, m2n)

    return jax.shard_map(device_step, mesh=mesh, in_specs=(row_spec, tok_spec, tok_spec, repl_spec, vocab_spec, repl_spec, repl_spec, vocab_spec, vocab_spec), out_specs=(tok_spec, P("dp"), row_spec, part_spec, part_spec, part_spec, row_spec, row_spec, row_spec), check_vma=False)
```

```python
import functools
import math

import jax
import jax.numpy as jnp
from jax import lax
from jax.experimental import pallas as pl
from jax.experimental.pallas import tpu as pltpu
from jax.sharding import PartitionSpec as P

LN_EPS = 1e-5
BETA_ONE = 0.9
BETA_TWO = 0.95
ADAM_EPS = 1e-8
LEARN_RATE = 1e-3
WEIGHT_DECAY = 0.1
ADAM_STEP = 10
MESH = pl.DeviceIdType.MESH
CORES = 2
PAIR = (0, 1)
TILE = 320
COPY_TILE = 272
ANY = pl.BlockSpec(memory_space=pl.ANY)
F32, BF16 = jnp.float32, jnp.bfloat16
NN = (((1,), (0,)), ((), ()))
NT = (((1,), (1,)), ((), ()))


def adam_step(param_val, grad_val, m_old, v_old, decay_rate):
    m_new = BETA_ONE * m_old + (1.0 - BETA_ONE) * grad_val
    v_new = BETA_TWO * v_old + (1.0 - BETA_TWO) * grad_val * grad_val
    m_hat = m_new / (1.0 - BETA_ONE ** ADAM_STEP)
    v_hat = v_new / (1.0 - BETA_TWO ** ADAM_STEP)
    new_param = param_val - LEARN_RATE * (m_hat / (jnp.sqrt(v_hat) + ADAM_EPS) + decay_rate * param_val)
    return new_param, m_new, v_new


def row_tiles(rows, size):
    return [(r, min(size, rows - r)) for r in range(0, rows, size)]


def step_kernel(side, hid_hbm, tgt_hbm, msk_hbm, lnp_hbm, emb_ref, m1_hbm, m2_hbm,
                e_out, m1_out, m2_out, dh_out, dln_out, sm_out,
                hid_ref, tgt_ref, msk_ref, lnp_ref, dh_buf, dln_buf, sm_buf,
                xg, ee, et, ez, dz, dxp, r1, r2, q1, q2,
                tm_all, st_all, tl_all, zb, tgt_ck, msk_ck, rel_ck, top_ck, lse_ck, s_ck, loss_ck, pair, dl_all,
                in_sem, out_sem, mom_sem, ag_s, ag1_r, ag2_r, ag3_r, tm_s, tm_r, st_s, st_r, tl_s, tl_r,
                rs_s, rs_r, ring_r, dl_s, dl_r, pr_s, pr_r, free_sem):
    chips = side * side
    ndev = chips * CORES
    tok, dim = hid_ref.shape
    half = tok // 2
    voc = emb_ref.shape[0]
    pairs = side // 2
    ct = 2 * tok
    nck = side * pairs
    hd, qd = dim // 2, dim // 4
    plus, minus = 1, side - 1
    me = lax.axis_index("tp")
    core = lax.rem(me, CORES)
    chip = me // CORES
    mx, my = lax.rem(chip, side), chip // side
    odd = lax.rem(mx, 2)
    sib = me + 1 - 2 * core

    def chip_at(dy, dx):
        return lax.rem(my + dy, side) * side + lax.rem(mx + dx, side)

    def rel(g, dmaj, dmin):
        return (dmin, dmaj) if g else (dmaj, dmin)

    def dev(g, dmaj, dmin):
        return {"tp": chip_at(*rel(g, dmaj, dmin)) * CORES + core}

    def rcopy(src, dst, ssem, rsem, device):
        return pltpu.make_async_remote_copy(src_ref=src, dst_ref=dst, send_sem=ssem, recv_sem=rsem,
                                            device_id=device, device_id_type=MESH)

    loads = [pltpu.make_async_copy(s, d, in_sem.at[i]) for i, (s, d) in enumerate(
        ((hid_hbm, hid_ref), (lnp_hbm, lnp_ref), (tgt_hbm, tgt_ref), (msk_hbm, msk_ref), (emb_ref, ee.at[0])))]
    for cp in loads:
        cp.start()
    barrier = pltpu.get_barrier_semaphore()
    for d in range(1, ndev):
        pl.semaphore_signal(barrier, inc=1, device_id={"tp": lax.rem(me + d, ndev)}, device_id_type=MESH)
    for cp in loads[:4]:
        cp.wait()

    def normalize():
        rows = hid_ref[...].astype(F32)
        cent = rows - jnp.mean(rows, axis=-1, keepdims=True)
        rstd = lax.rsqrt(jnp.mean(cent * cent, axis=-1, keepdims=True) + LN_EPS)
        return cent * rstd, rstd

    xb = (normalize()[0] * lnp_ref[0:1, :] + lnp_ref[1:2, :]).astype(BF16)

    def xslot(g, dmaj, dmin, r0=0, n=half):
        row = chip_at(*rel(g, dmaj, dmin)) * tok + g * half + r0
        return xg.at[pl.ds(pl.multiple_of(row, 32), n)]

    xg[pl.ds(pl.multiple_of(chip * tok, tok), tok), :] = xb
    tm_all[chip, 0:1, :] = tgt_ref[...]
    tm_all[chip, 1:2, :] = msk_ref[...]
    et[:, :, voc:] = jnp.zeros((2, dim, et.shape[2] - voc), BF16)
    dz[:, voc:, :] = jnp.zeros((2, dz.shape[1] - voc, dz.shape[2]), BF16)

    pl.semaphore_wait(barrier, ndev - 1)

    ways = (plus, minus)
    back = (minus, plus)

    def first(g, k, dmin=0):
        s = xslot(g, 0, dmin)
        return rcopy(s, s, ag_s, ag1_r.at[g, 0, k], dev(g, 0, ways[k]))

    def first_fwd(g, k, dmin):
        s = xslot(g, 0, dmin, k * (half // 2), half // 2)
        return rcopy(s, s, ag_s, ag1_r.at[g, 1, k], dev(g, 0, ways[k]))

    rel_pos = (0, minus, plus, 2)

    def second(g, r, k, dmaj=0):
        s = xslot(g, dmaj, rel_pos[r])
        return rcopy(s, s, ag_s, ag2_r.at[g, r, k], dev(g, ways[k], 0))

    def third(g, r, dmaj):
        s = xslot(g, dmaj, rel_pos[r])
        return rcopy(s, s, ag_s, ag3_r.at[g, r], dev(g, ways[r // 2], 0))

    def to_peers(ref, ssem, rsem):
        for d in range(1, chips):
            rcopy(ref, ref, ssem, rsem, {"tp": lax.rem(chip + d, chips) * CORES + core}).start()

    def all_of(ref, ssem, rsem):
        return rcopy(ref, ref, ssem, rsem, {"tp": sib})

    to_peers(tm_all.at[chip], tm_s, tm_r)
    tms = all_of(tm_all.at[pl.ds(0, chips - 1)], tm_s, tm_r)
    for g in PAIR:
        for k in PAIR:
            first(g, k).start()
    e_send = rcopy(emb_ref, ee.at[1], pr_s.at[0], pr_r.at[0], {"tp": sib})
    e_send.start()
    for g in PAIR:
        for k in PAIR:
            second(g, 0, k).start()

    for k in PAIR:
        for g in PAIR:
            first(g, k, back[k]).wait_recv()
            first_fwd(g, k, back[k]).start()
    for k in PAIR:
        for g in PAIR:
            for j in PAIR:
                second(g, 1 + k, j).start()

    def transpose_e(h):
        for r0, n in row_tiles(voc, 384):
            et[h, :, r0:r0 + n] = ee[h, r0:r0 + n, :].T

    loads[-1].wait()
    transpose_e(0)
    for g in PAIR:
        for k in PAIR:
            second(g, 0, k, back[k]).wait_recv()
        third(g, 0, minus).start()
    tms.wait_recv()
    for c in range(nck):
        for j in PAIR:
            v = tm_all[2 * c + j]
            tgt_ck[c:c + 1, j * tok:(j + 1) * tok] = v[0:1]
            msk_ck[c:c + 1, j * tok:(j + 1) * tok] = v[1:2]
    rel_ck[0] = tgt_ck[...] - me * voc
    rel_ck[1] = tgt_ck[...] - sib * voc
    maskf = msk_ck[...].astype(F32)
    pair[0] = jnp.broadcast_to(jnp.sum(maskf, keepdims=True), (8, tok))
    cnt_send = rcopy(pair.at[0], pair.at[1], pr_s.at[1], pr_r.at[1], {"tp": sib})
    cnt_send.start()
    e_send.wait_recv()
    transpose_e(1)

    tiles = [(h, r0, n) for h in PAIR for r0, n in row_tiles(voc, TILE)]

    def chunk_at(dy, dj):
        y, j = lax.rem(my + dy, side), lax.rem(mx // 2 + dj, pairs)
        return y * pairs + j, y, pl.multiple_of(j * ct, ct)

    def logits_chunk(dy, dj):
        c, i, lane0 = chunk_at(dy, dj)
        x_c = xg[pl.ds(pl.multiple_of(c * ct, ct), ct), :]
        tops, tots = [], []
        tl = jnp.zeros((1, ct), F32)

        def finish_tile(t):
            h, r0, n = tiles[t]
            z = zb[t % 2, :n, :]
            e = jnp.exp(z - tops[t])
            ez[i, h, r0:r0 + n, pl.ds(lane0, ct)] = e
            tots.append(jnp.sum(e, axis=0, keepdims=True))
            hit = lax.broadcasted_iota(jnp.int32, (n, ct), 0) == rel_ck[h, pl.ds(c, 1), :] - r0
            return jnp.sum(jnp.where(hit, z, 0.0), axis=0, keepdims=True)

        for t, (h, r0, n) in enumerate(tiles):
            z = lax.dot_general(ee[h, r0:r0 + n, :], x_c, NT, preferred_element_type=F32)
            zb[t % 2, :n, :] = z
            tops.append(jnp.max(z, axis=0, keepdims=True))
            if t:
                tl += finish_tile(t - 1)
        tl += finish_tile(len(tiles) - 1)
        top = functools.reduce(jnp.maximum, tops)
        tot = sum(s * jnp.exp(m - top) for m, s in zip(tops, tots))
        for t, m in enumerate(tops):
            top_ck[t, pl.ds(c, 1), :] = m
        tl_all[chip, pl.ds(c, 1), :] = tl
        st_all[c, chip] = top + jnp.log(tot)
        to_peers(st_all.at[c, chip], st_s, st_r.at[c])

    def gather1():
        for g in PAIR:
            for r in (1, 2):
                for k in PAIR:
                    second(g, r, k, back[k]).wait_recv()
                third(g, r, back[r // 2]).start()
        for g in PAIR:
            for k in PAIR:
                first_fwd(g, k, 2).wait_recv()
            for j in PAIR:
                second(g, 3, j).start()

    def gather3():
        for g in PAIR:
            third(g, 0, 2).wait_recv()

    def gather4():
        for g in PAIR:
            for k in PAIR:
                second(g, 3, k, back[k]).wait_recv()
            third(g, 3, plus).start()
        for g in PAIR:
            for r in (1, 2):
                third(g, r, 2).wait_recv()

    def gather7():
        for g in PAIR:
            third(g, 3, 2).wait_recv()

    def logits_step(k, carry):
        for i, event in ((1, gather1), (3, gather3), (4, gather4), (7, gather7)):
            pl.when(k == i)(event)
        far, t = k // 6, lax.rem(k, 3)
        logits_chunk((t + t // 2) * (1 - far) + 2 * far, (k // 3) * (1 - far) + (k - 6) * far)
        return carry

    lax.fori_loop(0, nck, logits_step, 0)
    to_peers(tl_all.at[chip], tl_s, tl_r)
    tls = all_of(tl_all.at[pl.ds(0, chips - 1)], tl_s, tl_r)
    cnt_send.wait_recv()
    total_n = (pair[0] + pair[1])[0:1, 0:1]
    s_ck[...] = maskf / total_n

    def grad_chunk(dy, dj):
        c, i, lane0 = chunk_at(dy, dj)
        out0 = pl.multiple_of(c * ct, ct)
        all_of(st_all.at[c, pl.ds(0, chips - 1)], st_s, st_r.at[c]).wait_recv()
        part = st_all[c]
        top = jnp.max(part, axis=0)
        lse = top + jnp.log(jnp.sum(jnp.exp(part - top[None]), axis=0))
        lse_ck[pl.ds(c, 1), :] = lse
        s = s_ck[pl.ds(c, 1), :]
        for t, (h, r0, n) in enumerate(tiles):
            a = jnp.exp(top_ck[t, pl.ds(c, 1), :] - lse) * s
            e = ez[i, h, r0:r0 + n, pl.ds(lane0, ct)]
            hit = lax.broadcasted_iota(jnp.int32, (n, ct), 0) == rel_ck[h, pl.ds(c, 1), :] - r0
            dz[h, r0:r0 + n, pl.ds(out0, ct)] = (e * a - jnp.where(hit, s, 0.0)).astype(BF16)
        for q in PAIR:
            acc = None
            for h in PAIR:
                t = lax.dot_general(et[h, q * hd:(q + 1) * hd, :], dz[h, :, pl.ds(out0, ct)], NN,
                                    preferred_element_type=F32)
                acc = t if acc is None else acc + t
            for j in PAIR:
                dxp[2 * c + j, q * hd:(q + 1) * hd, :] = acc[:, j * tok:(j + 1) * tok]

    hops = ((2, 0, 0, minus), (2, 1, 1, plus), (plus, 0, 1, plus), (minus, 1, 2, minus), (minus, 0, 0, minus), (plus, 1, 3, plus))

    def part(g, dmaj, dmin, q):
        return chip_at(*rel(g, dmaj, dmin)), pl.ds(g * hd + q * qd, qd)

    def ring1(g, s, k, hop=None):
        d, q, slot, to = hop or hops[k]
        src = dxp.at[chip_at(*rel(g, d, s)), pl.ds(g * hd + q * qd, qd)]
        land = r2 if hop or k > 1 else r1
        return rcopy(src, land.at[g, s, slot], rs_s, rs_r.at[g, s, 2 if hop or k > 1 else k], dev(g, to, 0))

    def direct1(g, s, b):
        ring1(g, s, 2 + b, (1 + 2 * b, b, 1 + b, 1 + 2 * b)).start()

    def relay1(g, s):
        for k in PAIR:
            ring1(g, s, k).wait_recv()
            i, q = part(g, ways[1 - k], s, k)
            dxp[i, q, :] = dxp[i, q, :] + r1[g, s, k]
            ring1(g, s, k + 4).start()

    def ring2(g, k):
        d, q, slot, to = hops[k]
        src = dxp.at[chip_at(*rel(g, 0, d)), pl.ds(g * hd + q * qd, qd)]
        return rcopy(src, (q1 if k < 2 else q2).at[g, slot], rs_s, ring_r.at[g, min(k, 2)], dev(g, 0, to))

    def finish1(s):
        for g in PAIR:
            all_of(r2.at[g, s], rs_s, rs_r.at[g, s, 2]).wait_recv()
            for q in PAIR:
                i, rows = part(g, 0, s, q)
                dxp[i, rows, :] = dxp[i, rows, :] + r2[g, s, 2 * q] + r2[g, s, 2 * q + 1]
            for k in {2: PAIR, plus: (2,), minus: (3,), 0: ()}[s]:
                ring2(g, k).start()

    def relay2():
        for k in PAIR:
            for g in PAIR:
                ring2(g, k).wait_recv()
                i, q = part(g, 0, ways[1 - k], k)
                dxp[i, q, :] = dxp[i, q, :] + q1[g, k]
                ring2(g, k + 4).start()

    near, far = 1 + 2 * odd, 3 - 2 * odd

    def grad_step(dy, dj):
        grad_chunk(dy, dj)
        for s in (2, far) if dj else (0, near):
            for k in {2: PAIR, plus: (2,), minus: (3,), 0: ()}[dy]:
                ring1(0, s, k).start()
        if dj:
            for k in PAIR:
                ring1(1, dy, k).start()
        direct1(1, dy, 1 - odd if dj else odd)

    grad_step(2, 0)
    grad_step(2, 1)
    grad_step(plus, 1)
    grad_step(minus, 1)
    grad_step(0, 1)
    relay1(0, 2)
    relay1(0, far)
    relay1(1, 2)
    grad_step(plus, 0)
    grad_step(minus, 0)
    relay1(0, near)
    relay1(1, plus)
    relay1(1, minus)
    relay1(0, 0)
    grad_step(0, 0)
    pl.semaphore_signal(free_sem, inc=1, device_id={"tp": sib}, device_id_type=MESH)

    def embed_grad(h, dst, t):
        r0, n = row_tiles(voc, 528)[t]
        ez[0, dst, r0:r0 + n, :] = lax.dot_general(dz[h, r0:r0 + n, :], xg[...], NN, preferred_element_type=F32)

    moments = [pltpu.make_async_copy(src, ez.at[2, i], mom_sem.at[i]) for i, src in enumerate((m1_hbm, m2_hbm))]
    for cp in moments:
        cp.start()
    embed_grad(1, 0, 0)
    relay1(1, 0)
    embed_grad(1, 0, 1)
    embed_grad(1, 0, 2)
    pl.semaphore_wait(free_sem, 1)
    de_send = rcopy(ez.at[0, 0], ez.at[1, 0], pr_s.at[3], pr_r.at[3], {"tp": sib})
    de_send.start()

    tls.wait_recv()
    loss = (lse_ck[...] - jnp.sum(tl_all[...], axis=0)) * maskf
    loss_ck[...] = loss
    pair[2] = jnp.broadcast_to(jnp.sum(loss, keepdims=True), (8, tok))
    loss_send = rcopy(pair.at[2], pair.at[3], pr_s.at[2], pr_r.at[2], {"tp": sib})
    loss_send.start()

    finish1(2)
    embed_grad(0, 1, 0)
    finish1(plus)
    finish1(minus)
    embed_grad(0, 1, 1)
    relay2()
    finish1(0)
    embed_grad(0, 1, 2)
    de_send.wait_recv()
    for cp in moments:
        cp.wait()
    writes = []
    for r0, n in row_tiles(voc, 528):
        sl = slice(r0, r0 + n)
        grad = ez[0, 1, sl, :] + ez[1, 0, sl, :]
        p, m1, m2 = adam_step(ee[0, sl, :].astype(F32), grad, ez[2, 0, sl, :], ez[2, 1, sl, :], WEIGHT_DECAY)
        ee[0, sl, :] = p.astype(BF16)
        ez[2, 0, sl, :] = m1
        ez[2, 1, sl, :] = m2
    for i, (src, dst) in enumerate(((ee.at[0], e_out), (ez.at[2, 0], m1_out), (ez.at[2, 1], m2_out))):
        writes.append(pltpu.make_async_copy(src, dst, mom_sem.at[i]))
        writes[-1].start()
    loss_send.wait_recv()
    sm_buf[...] = (pair[2] + pair[3]) / total_n
    row = loss_ck[pl.ds(chip // 2, 1), :]
    sm_buf[0:1, :] = jnp.where(odd == 0, row[:, :tok], row[:, tok:])
    sm_copy = pltpu.make_async_copy(sm_buf, sm_out, out_sem.at[1])
    sm_copy.start()

    for g in PAIR:
        all_of(q2.at[g], rs_s, ring_r.at[g, 2]).wait_recv()

    own = [dxp[chip, (2 * g + q) * qd:(2 * g + q + 1) * qd, :] + q2[g, 2 * q] + q2[g, 2 * q + 1] for g in PAIR for q in PAIR]
    dx = jnp.concatenate([v.T for v in own], axis=1)
    normed, rstd = normalize()
    dgam = jnp.sum(dx * normed, axis=0, keepdims=True)
    dbet = jnp.sum(dx, axis=0, keepdims=True)
    quarter = dim // tok
    for j in range(quarter):
        dl_all[me, j:j + 1, :] = dgam[:, j * tok:(j + 1) * tok]
        dl_all[me, quarter + j:quarter + j + 1, :] = dbet[:, j * tok:(j + 1) * tok]
    for d in range(1, ndev):
        rcopy(dl_all.at[me], dl_all.at[me], dl_s, dl_r, {"tp": lax.rem(me + d, ndev)}).start()
    dls = all_of(dl_all.at[pl.ds(0, ndev - 1)], dl_s, dl_r)
    dn = dx * lnp_ref[0:1, :]
    dh = rstd * (dn - jnp.mean(dn, axis=-1, keepdims=True) - normed * jnp.mean(dn * normed, axis=-1, keepdims=True))
    dh_buf[...] = dh.astype(BF16)
    dh_copy = pltpu.make_async_copy(dh_buf, dh_out, out_sem.at[2])
    dh_copy.start()

    blocks = 6 + 16 + 8
    all_of(xg.at[pl.ds(0, blocks * half)], ag_s, pr_r.at[0]).wait_send()
    all_of(dxp.at[pl.ds(0, 12 + 3)], rs_s, pr_r.at[0]).wait_send()
    all_of(st_all.at[:, pl.ds(0, chips - 1)], st_s, pr_r.at[0]).wait_send()
    for cp in (tms, tls, e_send, cnt_send, de_send, loss_send):
        cp.wait_send()

    dls.wait_recv()
    dl = jnp.sum(dl_all[...], axis=0)
    for j in range(quarter):
        for i in PAIR:
            dln_buf[i:i + 1, j * tok:(j + 1) * tok] = dl[i * quarter + j:i * quarter + j + 1]
    dln_copy = pltpu.make_async_copy(dln_buf, dln_out, out_sem.at[3])
    dln_copy.start()
    dls.wait_send()
    for cp in writes + [sm_copy, dh_copy, dln_copy]:
        cp.wait()


def finish_kernel(*refs):
    big_in, small_in, big_out = refs[:3], refs[3:9], refs[9:12]
    ln_new, lm1_new, lm2_new, loss_o, mean_o, dh_o = refs[12:18]
    scratch = refs[18:]
    big_buf, small_buf, ln_res, loss_res, mean_res = scratch[:3], scratch[3:9], scratch[9:12], scratch[12], scratch[13]
    in_sem, small_sem, out_sem, sout_sem = scratch[14:]
    tiles = row_tiles(big_in[0].shape[0], COPY_TILE)
    small = [pltpu.make_async_copy(s, d, small_sem.at[i]) for i, (s, d) in enumerate(zip(small_in, small_buf))]
    reads = [[pltpu.make_async_copy(s.at[pl.ds(r0, n)], d.at[pl.ds(r0, n)], in_sem.at[t, i])
              for i, (s, d) in enumerate(zip(big_in, big_buf))] for t, (r0, n) in enumerate(tiles)]
    for cp in reads[0] + small:
        cp.start()
    for row in reads[1:]:
        for cp in row:
            cp.start()
    for t, (r0, n) in enumerate(tiles):
        for i, (buf, dst) in enumerate(zip(big_buf, big_out)):
            reads[t][i].wait()
            pltpu.make_async_copy(buf.at[pl.ds(r0, n)], dst.at[pl.ds(r0, n)], out_sem.at[i]).start()
    for cp in small:
        cp.wait()
    dln, lnp, lm1, lm2, sm, dh = small_buf
    for buf, val in zip(ln_res, adam_step(lnp[...], dln[...], lm1[...], lm2[...], 0.0)):
        buf[...] = val
    loss_res[...] = sm[0:1, :]
    mean_res[...] = sm[1:2, 0:1]
    writes = []
    for i, (src, dst) in enumerate(zip((*ln_res, loss_res, mean_res, dh), (ln_new, lm1_new, lm2_new, loss_o, mean_o, dh_o))):
        writes.append(pltpu.make_async_copy(src, dst, sout_sem.at[i]))
        writes[-1].start()
    for i, buf in enumerate(big_buf):
        writes.append(pltpu.make_async_copy(buf, big_out[i], out_sem.at[i]))
    for cp in writes:
        cp.wait()


def solution(mesh):
    ntp = mesh.shape["tp"]
    side = math.isqrt(ntp // CORES)
    row_spec = P(("dp", "tp"), None)
    tok_spec = P(("dp", "tp"))
    vocab_spec = P("tp", None)
    repl_spec = P()
    part_spec = P("dp", None)

    def device_step(hidden, targets, loss_mask, ln_params, out_embed, ln_mom1, ln_mom2, embed_mom1, embed_mom2):
        tok, dim = hidden.shape
        voc = out_embed.shape[0]
        half, chips = tok // 2, side * side
        ct, nck, qd = 2 * tok, chips // 2, dim // 4
        ntok = ct * nck
        vpad = -(-voc // 128) * 128
        dma, vm = pltpu.SemaphoreType.DMA, pltpu.VMEM
        big = jax.ShapeDtypeStruct((voc, dim), F32)
        ln_s, sm_s = jax.ShapeDtypeStruct((2, dim), F32), jax.ShapeDtypeStruct((8, tok), F32)
        dh_s = jax.ShapeDtypeStruct((tok, dim), BF16)
        big_b = jax.ShapeDtypeStruct((voc, dim), BF16)
        e_new, m1n, m2n, dh, dln, sm = pl.pallas_call(
            functools.partial(step_kernel, side),
            out_shape=[big_b, big, big, dh_s, ln_s, sm_s],
            in_specs=[ANY] * 7,
            out_specs=[ANY] * 6,
            scratch_shapes=[
                vm((tok, dim), BF16), *[vm((1, tok), jnp.int32)] * 2, vm((2, dim), F32),
                vm((tok, dim), BF16), vm((2, dim), F32), vm((8, tok), F32),
                vm((ntok, dim), BF16),
                vm((2, voc, dim), BF16),
                vm((2, dim, vpad), BF16),
                vm((nck // 2, 2, voc, 2 * ct), F32),
                vm((2, vpad, ntok), BF16),
                vm((chips, dim, tok), F32),
                vm((2, side, 2, qd, tok), F32),
                vm((2, side, 4, qd, tok), F32),
                vm((2, 2, qd, tok), F32),
                vm((2, 4, qd, tok), F32),
                vm((chips, 2, tok), jnp.int32),
                vm((nck, chips, 1, ct), F32),
                vm((chips, nck, ct), F32),
                vm((2, TILE, ct), F32), *[vm((nck, ct), jnp.int32)] * 2, vm((2, nck, ct), jnp.int32),
                vm((2 * len(row_tiles(voc, TILE)), nck, ct), F32), *[vm((nck, ct), F32)] * 3,
                vm((4, 8, tok), F32),
                vm((ntp, 8, tok), F32),
                dma((5,)), dma((4,)), dma((3,)), dma(()), dma((2, 2, 2)), dma((2, 4, 2)), dma((2, 4)),
                dma(()), dma(()), dma(()), dma((nck,)), dma(()), dma(()),
                dma(()), dma((2, side, 3)), dma((2, 3)), dma(()), dma(()), *[dma((4,))] * 2,
                pltpu.SemaphoreType.REGULAR,
            ],
            compiler_params=pltpu.CompilerParams(collective_id=0, has_side_effects=True, vmem_limit_bytes=67043328),
            name="head_step",
        )(hidden, targets.reshape(1, tok), loss_mask.reshape(1, tok), ln_params, out_embed, embed_mom1, embed_mom2)

        nt = len(row_tiles(voc, COPY_TILE))
        bigs, smalls = [big_b, big, big], [ln_s, ln_s, ln_s, ln_s, sm_s, dh_s]
        outs = [ln_s, ln_s, ln_s, jax.ShapeDtypeStruct((1, tok), F32), jax.ShapeDtypeStruct((1, 1), F32), dh_s]
        e_new, m1n, m2n, lnn, lm1n, lm2n, loss, mean, dh = pl.pallas_call(
            finish_kernel,
            out_shape=bigs + outs,
            in_specs=[ANY] * 9,
            out_specs=[ANY] * 9,
            scratch_shapes=[vm(s.shape, s.dtype) for s in bigs + smalls + outs[:5]]
            + [dma((nt, 3)), dma((6,)), dma((3,)), dma((6,))],
            compiler_params=pltpu.CompilerParams(vmem_limit_bytes=67043328),
            name="finish",
        )(e_new, m1n, m2n, dln, ln_params, ln_mom1, ln_mom2, sm, dh)
        return (loss.reshape(tok), mean.reshape(1), dh, lnn, lm1n, lm2n, e_new, m1n, m2n)

    return jax.shard_map(device_step, mesh=mesh, in_specs=(row_spec, tok_spec, tok_spec, repl_spec, vocab_spec, repl_spec, repl_spec, vocab_spec, vocab_spec), out_specs=(tok_spec, P("dp"), row_spec, part_spec, part_spec, part_spec, row_spec, row_spec, row_spec), check_vma=False)
```

```python
import functools
import math

import jax
import jax.numpy as jnp
from jax import lax
from jax.experimental import pallas as pl
from jax.experimental.pallas import tpu as pltpu
from jax.sharding import PartitionSpec as P

LN_EPS = 1e-5
BETA_ONE = 0.9
BETA_TWO = 0.95
ADAM_EPS = 1e-8
LEARN_RATE = 1e-3
WEIGHT_DECAY = 0.1
ADAM_STEP = 10
MESH = pl.DeviceIdType.MESH
CORES = 2
PAIR = (0, 1)
TILE = 320
COPY_TILE = 272
ANY = pl.BlockSpec(memory_space=pl.ANY)
F32, BF16 = jnp.float32, jnp.bfloat16
NN = (((1,), (0,)), ((), ()))
NT = (((1,), (1,)), ((), ()))


def adam_step(param_val, grad_val, m_old, v_old, decay_rate):
    m_new = BETA_ONE * m_old + (1.0 - BETA_ONE) * grad_val
    v_new = BETA_TWO * v_old + (1.0 - BETA_TWO) * grad_val * grad_val
    m_hat = m_new / (1.0 - BETA_ONE ** ADAM_STEP)
    v_hat = v_new / (1.0 - BETA_TWO ** ADAM_STEP)
    new_param = param_val - LEARN_RATE * (m_hat / (jnp.sqrt(v_hat) + ADAM_EPS) + decay_rate * param_val)
    return new_param, m_new, v_new


def row_tiles(rows, size):
    return [(r, min(size, rows - r)) for r in range(0, rows, size)]


def step_kernel(side, hid_hbm, tgt_hbm, msk_hbm, lnp_hbm, emb_ref, m1_hbm, m2_hbm,
                e_out, m1_out, m2_out, dh_out, dln_out, sm_out,
                hid_ref, tgt_ref, msk_ref, lnp_ref, dh_buf, dln_buf, sm_buf,
                xg, ee, et, ez, dz, dxp, r1, r2, q1, q2,
                tm_all, st_all, tl_all, zb, tgt_ck, msk_ck, rel_ck, top_ck, lse_ck, s_ck, loss_ck, pair, dl_all,
                in_sem, out_sem, mom_sem, ag_s, ag1_r, ag2_r, ag3_r, tm_s, tm_r, st_s, st_r, tl_s, tl_r,
                rs_s, rs_r, ring_r, dl_s, dl_r, pr_s, pr_r, free_sem):
    chips = side * side
    ndev = chips * CORES
    tok, dim = hid_ref.shape
    half = tok // 2
    voc = emb_ref.shape[0]
    pairs = side // 2
    ct = 2 * tok
    nck = side * pairs
    hd, qd = dim // 2, dim // 4
    plus, minus = 1, side - 1
    me = lax.axis_index("tp")
    core = lax.rem(me, CORES)
    chip = me // CORES
    mx, my = lax.rem(chip, side), chip // side
    odd = lax.rem(mx, 2)
    sib = me + 1 - 2 * core

    def chip_at(dy, dx):
        return lax.rem(my + dy, side) * side + lax.rem(mx + dx, side)

    def rel(g, dmaj, dmin):
        return (dmin, dmaj) if g else (dmaj, dmin)

    def dev(g, dmaj, dmin):
        return {"tp": chip_at(*rel(g, dmaj, dmin)) * CORES + core}

    def rcopy(src, dst, ssem, rsem, device):
        return pltpu.make_async_remote_copy(src_ref=src, dst_ref=dst, send_sem=ssem, recv_sem=rsem,
                                            device_id=device, device_id_type=MESH)

    loads = [pltpu.make_async_copy(s, d, in_sem.at[i]) for i, (s, d) in enumerate(
        ((hid_hbm, hid_ref), (lnp_hbm, lnp_ref), (tgt_hbm, tgt_ref), (msk_hbm, msk_ref), (emb_ref, ee.at[0])))]
    for cp in loads:
        cp.start()
    barrier = pltpu.get_barrier_semaphore()
    for d in range(1, ndev):
        pl.semaphore_signal(barrier, inc=1, device_id={"tp": lax.rem(me + d, ndev)}, device_id_type=MESH)
    for cp in loads[:4]:
        cp.wait()

    def normalize():
        rows = hid_ref[...].astype(F32)
        cent = rows - jnp.mean(rows, axis=-1, keepdims=True)
        rstd = lax.rsqrt(jnp.mean(cent * cent, axis=-1, keepdims=True) + LN_EPS)
        return cent * rstd, rstd

    xb = (normalize()[0] * lnp_ref[0:1, :] + lnp_ref[1:2, :]).astype(BF16)

    def xslot(g, dmaj, dmin, r0=0, n=half):
        row = chip_at(*rel(g, dmaj, dmin)) * tok + g * half + r0
        return xg.at[pl.ds(pl.multiple_of(row, 32), n)]

    xg[pl.ds(pl.multiple_of(chip * tok, tok), tok), :] = xb
    tm_all[chip, 0:1, :] = tgt_ref[...]
    tm_all[chip, 1:2, :] = msk_ref[...]
    et[:, :, voc:] = jnp.zeros((2, dim, et.shape[2] - voc), BF16)
    dz[:, voc:, :] = jnp.zeros((2, dz.shape[1] - voc, dz.shape[2]), BF16)

    pl.semaphore_wait(barrier, ndev - 1)

    ways = (plus, minus)
    back = (minus, plus)

    def first(g, k, dmin=0):
        s = xslot(g, 0, dmin)
        return rcopy(s, s, ag_s, ag1_r.at[g, 0, k], dev(g, 0, ways[k]))

    def first_fwd(g, k, dmin):
        s = xslot(g, 0, dmin, k * (half // 2), half // 2)
        return rcopy(s, s, ag_s, ag1_r.at[g, 1, k], dev(g, 0, ways[k]))

    rel_pos = (0, minus, plus, 2)

    def second(g, r, k, dmaj=0):
        s = xslot(g, dmaj, rel_pos[r])
        return rcopy(s, s, ag_s, ag2_r.at[g, r, k], dev(g, ways[k], 0))

    def third(g, r, dmaj):
        s = xslot(g, dmaj, rel_pos[r])
        return rcopy(s, s, ag_s, ag3_r.at[g, r], dev(g, ways[r // 2], 0))

    def to_peers(ref, ssem, rsem):
        for d in range(1, chips):
            rcopy(ref, ref, ssem, rsem, {"tp": lax.rem(chip + d, chips) * CORES + core}).start()

    def all_of(ref, ssem, rsem):
        return rcopy(ref, ref, ssem, rsem, {"tp": sib})

    to_peers(tm_all.at[chip], tm_s, tm_r)
    tms = all_of(tm_all.at[pl.ds(0, chips - 1)], tm_s, tm_r)
    for g in PAIR:
        for k in PAIR:
            first(g, k).start()
    e_send = rcopy(emb_ref, ee.at[1], pr_s.at[0], pr_r.at[0], {"tp": sib})
    e_send.start()
    for g in PAIR:
        for k in PAIR:
            second(g, 0, k).start()

    for k in PAIR:
        for g in PAIR:
            first(g, k, back[k]).wait_recv()
            first_fwd(g, k, back[k]).start()
    for k in PAIR:
        for g in PAIR:
            for j in PAIR:
                second(g, 1 + k, j).start()

    def transpose_e(h):
        for r0, n in row_tiles(voc, 384):
            et[h, :, r0:r0 + n] = ee[h, r0:r0 + n, :].T

    loads[-1].wait()
    transpose_e(0)
    for g in PAIR:
        for k in PAIR:
            second(g, 0, k, back[k]).wait_recv()
        third(g, 0, minus).start()
    tms.wait_recv()
    for c in range(nck):
        for j in PAIR:
            v = tm_all[2 * c + j]
            tgt_ck[c:c + 1, j * tok:(j + 1) * tok] = v[0:1]
            msk_ck[c:c + 1, j * tok:(j + 1) * tok] = v[1:2]
    rel_ck[0] = tgt_ck[...] - me * voc
    rel_ck[1] = tgt_ck[...] - sib * voc
    maskf = msk_ck[...].astype(F32)
    pair[0] = jnp.broadcast_to(jnp.sum(maskf, keepdims=True), (8, tok))
    cnt_send = rcopy(pair.at[0], pair.at[1], pr_s.at[1], pr_r.at[1], {"tp": sib})
    cnt_send.start()
    e_send.wait_recv()
    transpose_e(1)

    tiles = [(h, r0, n) for h in PAIR for r0, n in row_tiles(voc, TILE)]

    def chunk_at(dy, dj):
        y, j = lax.rem(my + dy, side), lax.rem(mx // 2 + dj, pairs)
        return y * pairs + j, y, pl.multiple_of(j * ct, ct)

    def logits_chunk(dy, dj):
        c, i, lane0 = chunk_at(dy, dj)
        x_c = xg[pl.ds(pl.multiple_of(c * ct, ct), ct), :]
        tops, tots = [], []
        tl = jnp.zeros((1, ct), F32)

        def finish_tile(t):
            h, r0, n = tiles[t]
            z = zb[t % 2, :n, :]
            e = jnp.exp(z - tops[t])
            ez[i, h, r0:r0 + n, pl.ds(lane0, ct)] = e
            tots.append(jnp.sum(e, axis=0, keepdims=True))
            hit = lax.broadcasted_iota(jnp.int32, (n, ct), 0) == rel_ck[h, pl.ds(c, 1), :] - r0
            return jnp.sum(jnp.where(hit, z, 0.0), axis=0, keepdims=True)

        for t, (h, r0, n) in enumerate(tiles):
            z = lax.dot_general(ee[h, r0:r0 + n, :], x_c, NT, preferred_element_type=F32)
            zb[t % 2, :n, :] = z
            tops.append(jnp.max(z, axis=0, keepdims=True))
            if t:
                tl += finish_tile(t - 1)
        tl += finish_tile(len(tiles) - 1)
        top = functools.reduce(jnp.maximum, tops)
        tot = sum(s * jnp.exp(m - top) for m, s in zip(tops, tots))
        for t, m in enumerate(tops):
            top_ck[t, pl.ds(c, 1), :] = m
        tl_all[chip, pl.ds(c, 1), :] = tl
        st_all[c, chip] = top + jnp.log(tot)
        to_peers(st_all.at[c, chip], st_s, st_r.at[c])

    def gather1():
        for g in PAIR:
            for r in (1, 2):
                for k in PAIR:
                    second(g, r, k, back[k]).wait_recv()
                third(g, r, back[r // 2]).start()
        for g in PAIR:
            for k in PAIR:
                first_fwd(g, k, 2).wait_recv()
            for j in PAIR:
                second(g, 3, j).start()

    def gather3():
        for g in PAIR:
            third(g, 0, 2).wait_recv()

    def gather4():
        for g in PAIR:
            for k in PAIR:
                second(g, 3, k, back[k]).wait_recv()
            third(g, 3, plus).start()
        for g in PAIR:
            for r in (1, 2):
                third(g, r, 2).wait_recv()

    def gather7():
        for g in PAIR:
            third(g, 3, 2).wait_recv()

    def logits_step(k, carry):
        for i, event in ((1, gather1), (3, gather3), (4, gather4), (7, gather7)):
            pl.when(k == i)(event)
        far, t = k // 6, lax.rem(k, 3)
        logits_chunk((t + t // 2) * (1 - far) + 2 * far, (k // 3) * (1 - far) + (k - 6) * far)
        return carry

    lax.fori_loop(0, nck, logits_step, 0)
    to_peers(tl_all.at[chip], tl_s, tl_r)
    tls = all_of(tl_all.at[pl.ds(0, chips - 1)], tl_s, tl_r)
    cnt_send.wait_recv()
    total_n = (pair[0] + pair[1])[0:1, 0:1]
    s_ck[...] = maskf / total_n

    def grad_chunk(dy, dj):
        c, i, lane0 = chunk_at(dy, dj)
        out0 = pl.multiple_of(c * ct, ct)
        all_of(st_all.at[c, pl.ds(0, chips - 1)], st_s, st_r.at[c]).wait_recv()
        part = st_all[c]
        top = jnp.max(part, axis=0)
        lse = top + jnp.log(jnp.sum(jnp.exp(part - top[None]), axis=0))
        lse_ck[pl.ds(c, 1), :] = lse
        s = s_ck[pl.ds(c, 1), :]
        for t, (h, r0, n) in enumerate(tiles):
            a = jnp.exp(top_ck[t, pl.ds(c, 1), :] - lse) * s
            e = ez[i, h, r0:r0 + n, pl.ds(lane0, ct)]
            hit = lax.broadcasted_iota(jnp.int32, (n, ct), 0) == rel_ck[h, pl.ds(c, 1), :] - r0
            dz[h, r0:r0 + n, pl.ds(out0, ct)] = (e * a - jnp.where(hit, s, 0.0)).astype(BF16)
        for q in PAIR:
            acc = None
            for h in PAIR:
                t = lax.dot_general(et[h, q * hd:(q + 1) * hd, :], dz[h, :, pl.ds(out0, ct)], NN,
                                    preferred_element_type=F32)
                acc = t if acc is None else acc + t
            for j in PAIR:
                dxp[2 * c + j, q * hd:(q + 1) * hd, :] = acc[:, j * tok:(j + 1) * tok]

    hops = ((2, 0, 0, minus), (2, 1, 1, plus), (plus, 0, 1, plus), (minus, 1, 2, minus), (minus, 0, 0, minus), (plus, 1, 3, plus))

    def part(g, dmaj, dmin, q):
        return chip_at(*rel(g, dmaj, dmin)), pl.ds(g * hd + q * qd, qd)

    def ring1(g, s, k, hop=None):
        d, q, slot, to = hop or hops[k]
        src = dxp.at[chip_at(*rel(g, d, s)), pl.ds(g * hd + q * qd, qd)]
        land = r2 if hop or k > 1 else r1
        return rcopy(src, land.at[g, s, slot], rs_s, rs_r.at[g, s, 2 if hop or k > 1 else k], dev(g, to, 0))

    def direct1(g, s, b):
        ring1(g, s, 2 + b, (1 + 2 * b, b, 1 + b, 1 + 2 * b)).start()

    def relay1(g, s):
        for k in PAIR:
            ring1(g, s, k).wait_recv()
            i, q = part(g, ways[1 - k], s, k)
            dxp[i, q, :] = dxp[i, q, :] + r1[g, s, k]
            ring1(g, s, k + 4).start()

    def ring2(g, k):
        d, q, slot, to = hops[k]
        src = dxp.at[chip_at(*rel(g, 0, d)), pl.ds(g * hd + q * qd, qd)]
        return rcopy(src, (q1 if k < 2 else q2).at[g, slot], rs_s, ring_r.at[g, min(k, 2)], dev(g, 0, to))

    def finish1(s):
        for g in PAIR:
            all_of(r2.at[g, s], rs_s, rs_r.at[g, s, 2]).wait_recv()
            for q in PAIR:
                i, rows = part(g, 0, s, q)
                dxp[i, rows, :] = dxp[i, rows, :] + r2[g, s, 2 * q] + r2[g, s, 2 * q + 1]
            for k in {2: PAIR, plus: (2,), minus: (3,), 0: ()}[s]:
                ring2(g, k).start()

    def relay2():
        for k in PAIR:
            for g in PAIR:
                ring2(g, k).wait_recv()
                i, q = part(g, 0, ways[1 - k], k)
                dxp[i, q, :] = dxp[i, q, :] + q1[g, k]
                ring2(g, k + 4).start()

    near, far = 1 + 2 * odd, 3 - 2 * odd

    def grad_step(dy, dj):
        grad_chunk(dy, dj)
        for s in (2, far) if dj else (0, near):
            for k in {2: PAIR, plus: (2,), minus: (3,), 0: ()}[dy]:
                ring1(0, s, k).start()
        if dj:
            for k in PAIR:
                ring1(1, dy, k).start()
        direct1(1, dy, 1 - odd if dj else odd)

    grad_step(2, 1)
    grad_step(2, 0)
    grad_step(plus, 1)
    grad_step(minus, 1)
    grad_step(0, 1)
    relay1(0, 2)
    relay1(0, far)
    relay1(1, 2)
    grad_step(plus, 0)
    grad_step(minus, 0)
    relay1(0, near)
    relay1(1, plus)
    relay1(1, minus)
    relay1(0, 0)
    grad_step(0, 0)
    pl.semaphore_signal(free_sem, inc=1, device_id={"tp": sib}, device_id_type=MESH)

    def embed_grad(h, dst, t):
        r0, n = row_tiles(voc, 528)[t]
        ez[0, dst, r0:r0 + n, :] = lax.dot_general(dz[h, r0:r0 + n, :], xg[...], NN, preferred_element_type=F32)

    moments = [pltpu.make_async_copy(src, ez.at[2, i], mom_sem.at[i]) for i, src in enumerate((m1_hbm, m2_hbm))]
    for cp in moments:
        cp.start()
    embed_grad(1, 0, 0)
    relay1(1, 0)
    embed_grad(1, 0, 1)
    embed_grad(1, 0, 2)
    pl.semaphore_wait(free_sem, 1)
    de_send = rcopy(ez.at[0, 0], ez.at[1, 0], pr_s.at[3], pr_r.at[3], {"tp": sib})
    de_send.start()

    tls.wait_recv()
    loss = (lse_ck[...] - jnp.sum(tl_all[...], axis=0)) * maskf
    loss_ck[...] = loss
    pair[2] = jnp.broadcast_to(jnp.sum(loss, keepdims=True), (8, tok))
    loss_send = rcopy(pair.at[2], pair.at[3], pr_s.at[2], pr_r.at[2], {"tp": sib})
    loss_send.start()

    finish1(2)
    embed_grad(0, 1, 0)
    finish1(plus)
    finish1(minus)
    embed_grad(0, 1, 1)
    relay2()
    finish1(0)
    embed_grad(0, 1, 2)
    de_send.wait_recv()
    for cp in moments:
        cp.wait()
    writes = []
    for r0, n in row_tiles(voc, 528):
        sl = slice(r0, r0 + n)
        grad = ez[0, 1, sl, :] + ez[1, 0, sl, :]
        p, m1, m2 = adam_step(ee[0, sl, :].astype(F32), grad, ez[2, 0, sl, :], ez[2, 1, sl, :], WEIGHT_DECAY)
        ee[0, sl, :] = p.astype(BF16)
        ez[2, 0, sl, :] = m1
        ez[2, 1, sl, :] = m2
    for i, (src, dst) in enumerate(((ee.at[0], e_out), (ez.at[2, 0], m1_out), (ez.at[2, 1], m2_out))):
        writes.append(pltpu.make_async_copy(src, dst, mom_sem.at[i]))
        writes[-1].start()
    loss_send.wait_recv()
    sm_buf[...] = (pair[2] + pair[3]) / total_n
    row = loss_ck[pl.ds(chip // 2, 1), :]
    sm_buf[0:1, :] = jnp.where(odd == 0, row[:, :tok], row[:, tok:])
    sm_copy = pltpu.make_async_copy(sm_buf, sm_out, out_sem.at[1])
    sm_copy.start()

    for g in PAIR:
        all_of(q2.at[g], rs_s, ring_r.at[g, 2]).wait_recv()

    own = [dxp[chip, (2 * g + q) * qd:(2 * g + q + 1) * qd, :] + q2[g, 2 * q] + q2[g, 2 * q + 1] for g in PAIR for q in PAIR]
    dx = jnp.concatenate([v.T for v in own], axis=1)
    normed, rstd = normalize()
    dgam = jnp.sum(dx * normed, axis=0, keepdims=True)
    dbet = jnp.sum(dx, axis=0, keepdims=True)
    quarter = dim // tok
    for j in range(quarter):
        dl_all[me, j:j + 1, :] = dgam[:, j * tok:(j + 1) * tok]
        dl_all[me, quarter + j:quarter + j + 1, :] = dbet[:, j * tok:(j + 1) * tok]
    for d in range(1, ndev):
        rcopy(dl_all.at[me], dl_all.at[me], dl_s, dl_r, {"tp": lax.rem(me + d, ndev)}).start()
    dls = all_of(dl_all.at[pl.ds(0, ndev - 1)], dl_s, dl_r)
    dn = dx * lnp_ref[0:1, :]
    dh = rstd * (dn - jnp.mean(dn, axis=-1, keepdims=True) - normed * jnp.mean(dn * normed, axis=-1, keepdims=True))
    dh_buf[...] = dh.astype(BF16)
    dh_copy = pltpu.make_async_copy(dh_buf, dh_out, out_sem.at[2])
    dh_copy.start()

    blocks = 6 + 16 + 8
    all_of(xg.at[pl.ds(0, blocks * half)], ag_s, pr_r.at[0]).wait_send()
    all_of(dxp.at[pl.ds(0, 12 + 3)], rs_s, pr_r.at[0]).wait_send()
    all_of(st_all.at[:, pl.ds(0, chips - 1)], st_s, pr_r.at[0]).wait_send()
    for cp in (tms, tls, e_send, cnt_send, de_send, loss_send):
        cp.wait_send()

    dls.wait_recv()
    dl = jnp.sum(dl_all[...], axis=0)
    for j in range(quarter):
        for i in PAIR:
            dln_buf[i:i + 1, j * tok:(j + 1) * tok] = dl[i * quarter + j:i * quarter + j + 1]
    dln_copy = pltpu.make_async_copy(dln_buf, dln_out, out_sem.at[3])
    dln_copy.start()
    dls.wait_send()
    for cp in writes + [sm_copy, dh_copy, dln_copy]:
        cp.wait()


def finish_kernel(*refs):
    big_in, small_in, big_out = refs[:3], refs[3:9], refs[9:12]
    ln_new, lm1_new, lm2_new, loss_o, mean_o, dh_o = refs[12:18]
    scratch = refs[18:]
    big_buf, small_buf, ln_res, loss_res, mean_res = scratch[:3], scratch[3:9], scratch[9:12], scratch[12], scratch[13]
    in_sem, small_sem, out_sem, sout_sem = scratch[14:]
    tiles = row_tiles(big_in[0].shape[0], COPY_TILE)
    small = [pltpu.make_async_copy(s, d, small_sem.at[i]) for i, (s, d) in enumerate(zip(small_in, small_buf))]
    reads = [[pltpu.make_async_copy(s.at[pl.ds(r0, n)], d.at[pl.ds(r0, n)], in_sem.at[t, i])
              for i, (s, d) in enumerate(zip(big_in, big_buf))] for t, (r0, n) in enumerate(tiles)]
    for cp in reads[0] + small:
        cp.start()
    for row in reads[1:]:
        for cp in row:
            cp.start()
    for t, (r0, n) in enumerate(tiles):
        for i, (buf, dst) in enumerate(zip(big_buf, big_out)):
            reads[t][i].wait()
            pltpu.make_async_copy(buf.at[pl.ds(r0, n)], dst.at[pl.ds(r0, n)], out_sem.at[i]).start()
    for cp in small:
        cp.wait()
    dln, lnp, lm1, lm2, sm, dh = small_buf
    for buf, val in zip(ln_res, adam_step(lnp[...], dln[...], lm1[...], lm2[...], 0.0)):
        buf[...] = val
    loss_res[...] = sm[0:1, :]
    mean_res[...] = sm[1:2, 0:1]
    writes = []
    for i, (src, dst) in enumerate(zip((*ln_res, loss_res, mean_res, dh), (ln_new, lm1_new, lm2_new, loss_o, mean_o, dh_o))):
        writes.append(pltpu.make_async_copy(src, dst, sout_sem.at[i]))
        writes[-1].start()
    for i, buf in enumerate(big_buf):
        writes.append(pltpu.make_async_copy(buf, big_out[i], out_sem.at[i]))
    for cp in writes:
        cp.wait()


def solution(mesh):
    ntp = mesh.shape["tp"]
    side = math.isqrt(ntp // CORES)
    row_spec = P(("dp", "tp"), None)
    tok_spec = P(("dp", "tp"))
    vocab_spec = P("tp", None)
    repl_spec = P()
    part_spec = P("dp", None)

    def device_step(hidden, targets, loss_mask, ln_params, out_embed, ln_mom1, ln_mom2, embed_mom1, embed_mom2):
        tok, dim = hidden.shape
        voc = out_embed.shape[0]
        half, chips = tok // 2, side * side
        ct, nck, qd = 2 * tok, chips // 2, dim // 4
        ntok = ct * nck
        vpad = -(-voc // 128) * 128
        dma, vm = pltpu.SemaphoreType.DMA, pltpu.VMEM
        big = jax.ShapeDtypeStruct((voc, dim), F32)
        ln_s, sm_s = jax.ShapeDtypeStruct((2, dim), F32), jax.ShapeDtypeStruct((8, tok), F32)
        dh_s = jax.ShapeDtypeStruct((tok, dim), BF16)
        big_b = jax.ShapeDtypeStruct((voc, dim), BF16)
        e_new, m1n, m2n, dh, dln, sm = pl.pallas_call(
            functools.partial(step_kernel, side),
            out_shape=[big_b, big, big, dh_s, ln_s, sm_s],
            in_specs=[ANY] * 7,
            out_specs=[ANY] * 6,
            scratch_shapes=[
                vm((tok, dim), BF16), *[vm((1, tok), jnp.int32)] * 2, vm((2, dim), F32),
                vm((tok, dim), BF16), vm((2, dim), F32), vm((8, tok), F32),
                vm((ntok, dim), BF16),
                vm((2, voc, dim), BF16),
                vm((2, dim, vpad), BF16),
                vm((nck // 2, 2, voc, 2 * ct), F32),
                vm((2, vpad, ntok), BF16),
                vm((chips, dim, tok), F32),
                vm((2, side, 2, qd, tok), F32),
                vm((2, side, 4, qd, tok), F32),
                vm((2, 2, qd, tok), F32),
                vm((2, 4, qd, tok), F32),
                vm((chips, 2, tok), jnp.int32),
                vm((nck, chips, 1, ct), F32),
                vm((chips, nck, ct), F32),
                vm((2, TILE, ct), F32), *[vm((nck, ct), jnp.int32)] * 2, vm((2, nck, ct), jnp.int32),
                vm((2 * len(row_tiles(voc, TILE)), nck, ct), F32), *[vm((nck, ct), F32)] * 3,
                vm((4, 8, tok), F32),
                vm((ntp, 8, tok), F32),
                dma((5,)), dma((4,)), dma((3,)), dma(()), dma((2, 2, 2)), dma((2, 4, 2)), dma((2, 4)),
                dma(()), dma(()), dma(()), dma((nck,)), dma(()), dma(()),
                dma(()), dma((2, side, 3)), dma((2, 3)), dma(()), dma(()), *[dma((4,))] * 2,
                pltpu.SemaphoreType.REGULAR,
            ],
            compiler_params=pltpu.CompilerParams(collective_id=0, has_side_effects=True, vmem_limit_bytes=67043328),
            name="head_step",
        )(hidden, targets.reshape(1, tok), loss_mask.reshape(1, tok), ln_params, out_embed, embed_mom1, embed_mom2)

        nt = len(row_tiles(voc, COPY_TILE))
        bigs, smalls = [big_b, big, big], [ln_s, ln_s, ln_s, ln_s, sm_s, dh_s]
        outs = [ln_s, ln_s, ln_s, jax.ShapeDtypeStruct((1, tok), F32), jax.ShapeDtypeStruct((1, 1), F32), dh_s]
        e_new, m1n, m2n, lnn, lm1n, lm2n, loss, mean, dh = pl.pallas_call(
            finish_kernel,
            out_shape=bigs + outs,
            in_specs=[ANY] * 9,
            out_specs=[ANY] * 9,
            scratch_shapes=[vm(s.shape, s.dtype) for s in bigs + smalls + outs[:5]]
            + [dma((nt, 3)), dma((6,)), dma((3,)), dma((6,))],
            compiler_params=pltpu.CompilerParams(vmem_limit_bytes=67043328),
            name="finish",
        )(e_new, m1n, m2n, dln, ln_params, ln_mom1, ln_mom2, sm, dh)
        return (loss.reshape(tok), mean.reshape(1), dh, lnn, lm1n, lm2n, e_new, m1n, m2n)

    return jax.shard_map(device_step, mesh=mesh, in_specs=(row_spec, tok_spec, tok_spec, repl_spec, vocab_spec, repl_spec, repl_spec, vocab_spec, vocab_spec), out_specs=(tok_spec, P("dp"), row_spec, part_spec, part_spec, part_spec, row_spec, row_spec, row_spec), check_vma=False)
```
